128 devices in a mesh: keys: 32 (over y, z, core), view: 4 (over x).
Axes of the slice: x: 4, y: 4, z: 4, core: 2. Of those that a mesh axis runs over, the one named last changes fastest.
Arguments:
- key_slot: int32 [16384], replicated, may hold values from 0 to 16383, as said below
- a_slot: int32 [524288], P(('keys', 'view')), may hold values from 0 to 511
- a_group: int32 [524288], P(('keys', 'view')), may hold values from 0 to 4095
- a_weight: int32 [524288], P(('keys', 'view')), may hold values from 1 to 3
- a_payload: bfloat16 [524288, 256], P(('keys', 'view')), may hold values from -1.1953125 to 1.1953125
- b_slot: int32 [524288], P(('keys', 'view')), may hold values from 0 to 511
- b_weight: int32 [524288], P(('keys', 'view')), may hold values from 1 to 3
- b_payload: bfloat16 [524288, 256], P(('keys', 'view')), may hold values from -0.59765625 to 0.59765625
- da_key: int32 [131072], P(('keys', 'view')), may hold values from 0 to 16383, as said below
- da_group: int32 [131072], P(('keys', 'view')), may hold values from 0 to 4095
- da_mult: int32 [131072], P(('keys', 'view')), may hold values from -1 to 1, as said below
- da_payload: bfloat16 [131072, 256], P(('keys', 'view')), may hold values from -1.796875 to 1.796875
- da_count: int32 [128], P(('keys', 'view')), may hold values from 768 to 1024, as said below
- db_key: int32 [131072], P(('keys', 'view')), may hold values from 0 to 16383, as said below
- db_mult: int32 [131072], P(('keys', 'view')), may hold values from -1 to 1, as said below
- db_payload: bfloat16 [131072, 256], P(('keys', 'view')), may hold values from -1.1953125 to 1.1953125
- db_count: int32 [128], P(('keys', 'view')), may hold values from 768 to 1024, as said below
Outputs:
- view_delta: float32 [4096, 256], P(('keys', 'view'))
The draws below stay inside these ranges and needn't reach their ends.
Inputs may be any that keep to these rules, and one draw needn't show every extreme that they name: `key_slot`: A permutation of 0 to 16383. `da_key`: among the 1024 slots of one device, at most 64 have keys held by one keys index; in every draw one keys index gets exactly 64 live rows from every device. `db_key`: among the 1024 slots of one device, at most 64 have keys held by one keys index; in every draw one keys index gets exactly 64 live rows from every device. `da_mult`: each entry is -1 or 1. `db_mult`: each entry is -1 or 1. `da_count`: some device has all 1024 rows live. `db_count`: some device has all 1024 rows live.
All inputs are finite; a program needn't handle non-finite values.
Results may differ from the reference program's by a relative error of at most 0.0029.
Values may be sent and summed in bfloat16 or wider, within the bound.
No kernel may reach another device: no remote copies, remote signals or barrier semaphores. Data moves between devices by JAX's collectives and lax.ppermute only.
A program may use at most 64 MiB of HBM per device.

```python
import jax
import jax.numpy as jnp

D = 256
KEYS_DEV = 512
GROUPS_DEV = 32
A_DEV = 4096
B_DEV = 4096
DELTA_DEV = 1024
CAP = 64
KEYS = 16384
GROUPS = 4096
A_ROWS = 524288
B_ROWS = 524288
DELTA_ROWS = 131072
N_KEYS = 32
N_VIEW = 4


def draw_key_slot(key, part):
    return jax.random.permutation(jax.random.fold_in(key, 11), KEYS).astype(jnp.int32)


def delta_keys(key, salt_value):
    order = draw_key_slot(key, 0)
    inverse = jnp.zeros((KEYS,), jnp.int32).at[order].set(jnp.arange(KEYS, dtype=jnp.int32))
    base = jax.random.fold_in(key, salt_value)
    hot_owner = jax.random.randint(jax.random.fold_in(base, 1), (), 0, N_KEYS).astype(jnp.int32)
    others = (hot_owner + 1 + jnp.arange(N_KEYS - 1, dtype=jnp.int32)) % N_KEYS
    target_pool = jnp.repeat(others, CAP, total_repeat_length=(N_KEYS - 1) * CAP)
    device_keys = jax.random.split(jax.random.fold_in(base, 2), N_KEYS * N_VIEW)

    def one_device(device_key):
        shuffled = jax.random.permutation(jax.random.fold_in(device_key, 3), target_pool)
        target = jnp.concatenate([jnp.full((CAP,), hot_owner, jnp.int32), shuffled[:DELTA_DEV - CAP]])
        within = jax.random.randint(jax.random.fold_in(device_key, 4), (DELTA_DEV,), 0, KEYS_DEV).astype(jnp.int32)
        return jnp.take(inverse, target * KEYS_DEV + within)
    return jax.vmap(one_device)(device_keys).reshape(-1).astype(jnp.int32)


def delta_signs(key, salt_value):
    picked = jax.random.randint(jax.random.fold_in(key, salt_value), (DELTA_ROWS,), 0, 2)
    return (2 * picked - 1).astype(jnp.int32)


def delta_counts(key, salt_value):
    devices = N_KEYS * N_VIEW
    counts = jax.random.randint(jax.random.fold_in(key, salt_value), (devices,), 3 * DELTA_DEV // 4, DELTA_DEV + 1)
    full_device = jax.random.randint(jax.random.fold_in(key, salt_value + 1), (), 0, devices)
    return counts.at[full_device].set(DELTA_DEV).astype(jnp.int32)


def draw_da_key(key, part):
    return delta_keys(key, 21)


def draw_db_key(key, part):
    return delta_keys(key, 22)


def draw_da_mult(key, part):
    return delta_signs(key, 31)


def draw_db_mult(key, part):
    return delta_signs(key, 32)


def draw_da_count(key, part):
    return delta_counts(key, 41)


def draw_db_count(key, part):
    return delta_counts(key, 51)


def plant(entries, own_key, smallest, high):
    dims = entries.shape
    place = [jax.random.randint(jax.random.fold_in(own_key, axis), (), 0, dims[axis]) for axis in range(len(dims))]
    entries = entries.at[tuple(place)].set(smallest)
    longest = dims.index(max(dims))
    place[longest] = (place[longest] + 1) % dims[longest]
    return entries.at[tuple(place)].set(high)


def block_scale(key, dims, pieces, least, high):
    gain = 1.0
    for axis_at, shards_of in pieces:
        heights = jax.random.uniform(jax.random.fold_in(jax.random.fold_in(key, 6), axis_at), (shards_of,), jnp.float32, least / len(pieces), high / len(pieces))
        gain = gain * jnp.repeat(jnp.exp(heights), dims[axis_at] // shards_of).reshape((-1,) + (1,) * (len(dims) - 1 - axis_at))
    return gain


def scatter_about(key, shape, width, bound, cuts=(), held_as=jnp.bfloat16):
    result = width * jax.random.normal(key, shape, jnp.float32)
    if cuts:
        result = result * block_scale(key, shape, cuts, -0.22, 0.18)
    return jnp.clip(result, -bound, bound).astype(held_as)


def setup_inputs(seed: int = 0) -> dict:
    splits = jax.random.split(jax.random.key(seed), 18)
    key_slot = draw_key_slot(jax.random.fold_in(splits[17], 71), 0)
    a_slot = plant(jax.random.randint(splits[1], (A_ROWS,), 0, KEYS_DEV), jax.random.fold_in(splits[1], 1), 0, KEYS_DEV - 1).astype(jnp.int32)
    a_group = plant(jax.random.randint(splits[2], (A_ROWS,), 0, GROUPS), jax.random.fold_in(splits[2], 1), 0, GROUPS - 1).astype(jnp.int32)
    a_weight = plant(jax.random.randint(splits[3], (A_ROWS,), 1, 4), jax.random.fold_in(splits[3], 1), 1, 3).astype(jnp.int32)
    a_payload = scatter_about(splits[4], (A_ROWS, D), 0.2, 1.1953125, ((0, 128),))
    b_slot = plant(jax.random.randint(splits[5], (B_ROWS,), 0, KEYS_DEV), jax.random.fold_in(splits[5], 1), 0, KEYS_DEV - 1).astype(jnp.int32)
    b_weight = plant(jax.random.randint(splits[6], (B_ROWS,), 1, 4), jax.random.fold_in(splits[6], 1), 1, 3).astype(jnp.int32)
    b_payload = scatter_about(splits[7], (B_ROWS, D), 0.1, 0.59765625, ((0, 128),))
    da_key = draw_da_key(jax.random.fold_in(splits[17], 71), 0)
    da_group = plant(jax.random.randint(splits[9], (DELTA_ROWS,), 0, GROUPS), jax.random.fold_in(splits[9], 1), 0, GROUPS - 1).astype(jnp.int32)
    da_mult = draw_da_mult(jax.random.fold_in(splits[17], 71), 0)
    da_payload = scatter_about(splits[11], (DELTA_ROWS, D), 0.3, 1.796875, ((0, 128),))
    da_count = draw_da_count(jax.random.fold_in(splits[17], 71), 0)
    db_key = draw_db_key(jax.random.fold_in(splits[17], 71), 0)
    db_mult = draw_db_mult(jax.random.fold_in(splits[17], 71), 0)
    db_payload = scatter_about(splits[15], (DELTA_ROWS, D), 0.2, 1.1953125, ((0, 128),))
    db_count = draw_db_count(jax.random.fold_in(splits[17], 71), 0)
    return dict(key_slot=key_slot, a_slot=a_slot, a_group=a_group, a_weight=a_weight, a_payload=a_payload, b_slot=b_slot, b_weight=b_weight, b_payload=b_payload, da_key=da_key, da_group=da_group, da_mult=da_mult, da_payload=da_payload, da_count=da_count, db_key=db_key, db_mult=db_mult, db_payload=db_payload, db_count=db_count)


def reference(key_slot, a_slot, a_group, a_weight, a_payload, b_slot, b_weight, b_payload, da_key, da_group, da_mult, da_payload, da_count, db_key, db_mult, db_payload, db_count):
    devices = N_KEYS * N_VIEW
    total_keys = KEYS_DEV * N_KEYS
    total_groups = GROUPS_DEV * devices

    def owner_slots(local_slot, rows_dev):
        device_index = jnp.arange(local_slot.shape[0], dtype=jnp.int32) // rows_dev
        return (device_index // N_VIEW) * KEYS_DEV + local_slot

    def signed_rows(row_mult, row_count):
        position = jnp.arange(DELTA_DEV * devices, dtype=jnp.int32)
        alive_rows = (position % DELTA_DEV) < jnp.take(row_count, position // DELTA_DEV)
        return (row_mult * alive_rows.astype(jnp.int32)).astype(jnp.float32)

    key_b = jax.ops.segment_sum(b_weight[:, None].astype(jnp.float32) * b_payload.astype(jnp.float32), owner_slots(b_slot, B_DEV), num_segments=total_keys)
    key_db = jax.ops.segment_sum(signed_rows(db_mult, db_count)[:, None] * db_payload.astype(jnp.float32), jnp.take(key_slot, db_key), num_segments=total_keys)
    a_terms = (a_weight[:, None].astype(jnp.float32) * a_payload.astype(jnp.float32) * jnp.take(key_db, owner_slots(a_slot, A_DEV), axis=0)).astype(jnp.bfloat16)
    whole_table = key_b + key_db
    delta_terms = (signed_rows(da_mult, da_count)[:, None] * da_payload.astype(jnp.float32) * jnp.take(whole_table, jnp.take(key_slot, da_key), axis=0)).astype(jnp.bfloat16)
    view_delta = jax.ops.segment_sum(a_terms.astype(jnp.float32), a_group, num_segments=total_groups)
    view_delta = view_delta + jax.ops.segment_sum(delta_terms.astype(jnp.float32), da_group, num_segments=total_groups)
    return view_delta
```

```python
import jax
import jax.numpy as jnp
from jax import lax
from jax.experimental import pallas as pl
from jax.experimental.pallas import tpu as pltpu
from jax.sharding import Mesh
from jax.sharding import PartitionSpec as P

KEYS_DEV = 512
GROUPS_DEV = 32
GROUPS = 4096
DELTA_DEV = 1024
A_DEV = 4096
D = 256
OWNERS = 32
CAP = 64
BLOCK = CAP + 8
KEYS = ("keys_0", "keys_1", "keys_2")
KEYS_VIEW = ("keys_0", "keys_1", "keys_2", "view")
F32, BF16, I32 = jnp.float32, jnp.bfloat16, jnp.int32
NN = (((1,), (0,)), ((), ()))
NT = (((1,), (1,)), ((), ()))
TN = (((0,), (0,)), ((), ()))
VMEM = pl.BlockSpec(memory_space=pltpu.VMEM)
SMEM = pl.BlockSpec(memory_space=pltpu.SMEM)


def dot(x, y, dims=NN):
    return lax.dot_general(x, y, dims, preferred_element_type=F32)


def rows_of(shape):
    return lax.broadcasted_iota(I32, shape, 0)


def lanes_of(shape):
    return lax.broadcasted_iota(I32, shape, 1)


def flat(x):
    return jnp.concatenate([x[j : j + 1, :] for j in range(x.shape[0])], axis=1)


def pick(condition, value):
    return jnp.where(condition, value, 0.0).astype(BF16)


def pack_kernel(with_group, me_ref, count_ref, table_ref, key_ref, mult_ref, *rest):
    group_ref = rest[0] if with_group else None
    payload_ref, out_ref = rest[-2:]
    rows = DELTA_DEV
    key = flat(key_ref[...])
    key_hi, key_lo = key >> 7, key & 127
    low = pick(rows_of((128, rows)) == key_lo, 1.0)
    table = table_ref[...]
    found = dot((table >> 7).astype(F32).astype(BF16), low) * 128.0 + dot(
        (table & 127).astype(F32).astype(BF16), low
    )
    slot = jnp.sum(jnp.where(rows_of((128, rows)) == key_hi, found, 0.0), axis=0, keepdims=True)
    slot = slot.astype(I32)
    owner, local = slot >> 9, slot & 511
    live = lanes_of((1, rows)) < count_ref[0]
    owner = jnp.where(live, owner, -1)
    marks = jnp.where(rows_of((OWNERS, rows)) == owner, 1.0, 0.0)
    step = jnp.where(
        (rows_of((128, 256)) < lanes_of((128, 256))) | (lanes_of((128, 256)) >= 128), 1.0, 0.0
    ).astype(BF16)
    before, carry = [], jnp.zeros((OWNERS, 128), F32)
    for j in range(rows // 128):
        counted = dot(marks[:, 128 * j : 128 * (j + 1)].astype(BF16), step)
        before.append(counted[:, :128] + carry)
        carry = carry + counted[:, 128:]
    rank = jnp.sum(marks * jnp.concatenate(before, axis=1), axis=0, keepdims=True).astype(I32)
    position = jnp.where(live, owner * CAP + rank, -1)
    sign = flat(mult_ref[...]).astype(F32)
    payload = payload_ref[...]
    for c in range(OWNERS // 4):
        chosen = pick(rows_of((4 * CAP, rows)) + 4 * CAP * c == position, sign)
        packed = dot(chosen, payload).astype(BF16)
        for j in range(4):
            out_ref[pl.ds((4 * c + j) * BLOCK, CAP), :] = packed[CAP * j : CAP * (j + 1)]
    field = rows_of((8, rows))
    value = jnp.where(field == 0, local & 255, jnp.where(field == 1, local >> 8, 0))
    if with_group:
        group = flat(group_ref[...])
        value = jnp.where(field == 2, group & 255, jnp.where(field == 3, group >> 8, value))
    value = jnp.broadcast_to(value.astype(F32)[None], (OWNERS, 8, rows)).reshape(8 * OWNERS, rows)
    sent = pick((rows_of((8 * OWNERS, rows)) >> 3) == owner, value)
    place = pick(rows_of((4 * CAP, rows)) == rank + CAP * (me_ref[0] % 4), 1.0)
    fields = dot(sent, place, NT).astype(BF16)
    for k in range(OWNERS):
        out_ref[pl.ds(k * BLOCK + CAP, 8), :] = fields[8 * k : 8 * k + 8]


def pack(me, count, table, key, mult, group, payload):
    extra = [] if group is None else [group.reshape(8, 128)]
    return pl.pallas_call(
        lambda *refs: pack_kernel(group is not None, *refs),
        out_shape=jax.ShapeDtypeStruct((OWNERS * BLOCK, D), BF16),
        in_specs=[SMEM, SMEM] + [VMEM] * (4 + len(extra)),
        out_specs=VMEM,
        name="pack_a" if extra else "pack_b",
    )(me, count, table, key.reshape(8, 128), mult.reshape(8, 128), *extra, payload)


def fields_of(ref, c):
    total = ref[pl.ds(4 * c * BLOCK + CAP, 8), :].astype(F32)
    for j in range(1, 4):
        total = total + ref[pl.ds((4 * c + j) * BLOCK + CAP, 8), :].astype(F32)
    total = total.astype(I32)
    return total[0:1] + 256 * total[1:2], total[2:3] + 256 * total[3:4]


def payload_of(ref, c):
    return jnp.concatenate(
        [ref[pl.ds((4 * c + j) * BLOCK, CAP), :] for j in range(4)], axis=0
    )


def spread(total_ref, view, outs):
    for s in range(4):
        outs[s][...] = total_ref[pl.ds(((view + s) % 4) * 128, 128), :]


def sum_b_kernel(view_ref, slot_ref, weight_ref, payload_ref, *rest):
    outs, total_ref = rest[:4], rest[4]
    total_ref[...] = jnp.zeros_like(total_ref)
    for c in range(4):
        slot = flat(slot_ref[8 * c : 8 * c + 8, :])
        weight = flat(weight_ref[8 * c : 8 * c + 8, :]).astype(F32)
        chosen = pick(rows_of((KEYS_DEV, 1024)) == slot, weight)
        total_ref[...] += dot(chosen, payload_ref[1024 * c : 1024 * (c + 1), :])
    spread(total_ref, view_ref[0], outs)


def sum_db_kernel(view_ref, in_ref, *rest):
    outs, total_ref = rest[:4], rest[4]
    total_ref[...] = jnp.zeros_like(total_ref)
    for c in range(8):
        slot, _ = fields_of(in_ref, c)
        chosen = pick(rows_of((KEYS_DEV, 256)) == slot, 1.0)
        total_ref[...] += dot(chosen, payload_of(in_ref, c))
    spread(total_ref, view_ref[0], outs)


def slices(kernel, name, view, *args):
    return pl.pallas_call(
        kernel,
        out_shape=[jax.ShapeDtypeStruct((128, D), F32)] * 4,
        in_specs=[SMEM] + [VMEM] * len(args),
        out_specs=[VMEM] * 4,
        scratch_shapes=[pltpu.VMEM((KEYS_DEV, D), F32)],
        name=name,
    )(view, *args)


def shift(x, s):
    return lax.ppermute(x, "view", [(j, (j + s) % 4) for j in range(4)])


def own_total(parts):
    got = [parts[0]] + [shift(parts[s], s) for s in (1, 2, 3)]
    return (got[0] + got[1]) + (got[2] + got[3])


def everyone(x):
    return [x] + [shift(x, s) for s in (1, 2, 3)]


def join_kernel(view_ref, *refs):
    db, b = refs[:4], refs[4:8]
    slot_ref, group_ref, weight_ref, payload_ref, in_ref = refs[8:13]
    out_ref, table_ref, whole_ref, term_ref, groups_ref = refs[13:]
    view = view_ref[0]
    for s in range(4):
        at = pl.ds(((view + 4 - s) % 4) * 128, 128)
        table = db[s][...]
        whole = b[s][...] + table
        for ref, value in ((table_ref, table), (whole_ref, whole)):
            high = value.astype(BF16)
            ref[at, :D] = high
            ref[at, D:] = (value - high.astype(F32)).astype(BF16)

    def terms(ref, slot, weight, payload):
        chosen = pick(rows_of((KEYS_DEV, 256)) == slot, weight)
        got = dot(chosen, ref[...], TN)
        return (payload.astype(F32) * (got[:, :D] + got[:, D:])).astype(BF16)

    for c in range(16):
        slot = flat(slot_ref[2 * c : 2 * c + 2, :])
        weight = flat(weight_ref[2 * c : 2 * c + 2, :]).astype(F32)
        at = pl.ds(256 * c, 256)
        term_ref[at, :] = terms(table_ref, slot, weight, payload_ref[at, :])
        groups_ref[:, at] = flat(group_ref[2 * c : 2 * c + 2, :])
    for c in range(8):
        slot, group = fields_of(in_ref, c)
        at = pl.ds(A_DEV + 256 * c, 256)
        term_ref[at, :] = terms(whole_ref, slot, 1.0, payload_of(in_ref, c))
        groups_ref[:, at] = group

    def block(g, carry):
        rows = groups_ref.shape[1]
        chosen = pick(rows_of((256, rows)) + 256 * g == groups_ref[...], 1.0)
        out_ref[pl.ds(256 * g, 256), :] = dot(chosen, term_ref[...]).astype(BF16)
        return carry

    lax.fori_loop(0, GROUPS // 256, block, 0)


def join(view, db, b, slot, group, weight, payload, received):
    rows = A_DEV + OWNERS * CAP
    return pl.pallas_call(
        join_kernel,
        out_shape=jax.ShapeDtypeStruct((GROUPS, D), BF16),
        in_specs=[SMEM] + [VMEM] * 13,
        out_specs=VMEM,
        scratch_shapes=[
            pltpu.VMEM((KEYS_DEV, 2 * D), BF16),
            pltpu.VMEM((KEYS_DEV, 2 * D), BF16),
            pltpu.VMEM((rows, D), BF16),
            pltpu.VMEM((1, rows), I32),
        ],
        name="join",
    )(
        view, *db, *b, slot.reshape(32, 128), group.reshape(32, 128), weight.reshape(32, 128),
        payload, received,
    )


def exchange(packed):
    blocks = packed.reshape(OWNERS, BLOCK, D)
    return lax.all_to_all(blocks, KEYS, 0, 0, tiled=True).reshape(OWNERS * BLOCK, D)


def shards(
    key_slot,
    a_slot,
    a_group,
    a_weight,
    a_payload,
    b_slot,
    b_weight,
    b_payload,
    da_key,
    da_group,
    da_mult,
    da_payload,
    da_count,
    db_key,
    db_mult,
    db_payload,
    db_count,
):
    me = lax.axis_index(KEYS).astype(I32).reshape(1)
    view = lax.axis_index("view").astype(I32).reshape(1)
    table = key_slot.reshape(128, 128)
    db_in = exchange(pack(me, db_count, table, db_key, db_mult, None, db_payload))
    da_in = exchange(pack(me, da_count, table, da_key, da_mult, da_group, da_payload))
    b_parts = slices(
        sum_b_kernel, "sum_b", view, b_slot.reshape(32, 128), b_weight.reshape(32, 128), b_payload
    )
    b = everyone(own_total(b_parts))
    db = everyone(own_total(slices(sum_db_kernel, "sum_db", view, db_in)))
    partial = join(view, db, b, a_slot, a_group, a_weight, a_payload, da_in)
    blocks = partial.reshape(GROUPS // GROUPS_DEV, GROUPS_DEV, D)
    blocks = lax.all_to_all(blocks, KEYS_VIEW, 0, 0, tiled=True)
    return jnp.sum(blocks.astype(F32), axis=0)


def solution(mesh):
    split = Mesh(
        mesh.devices.reshape(4, 4, 2, mesh.shape["view"]), ("keys_0", "keys_1", "keys_2", "view")
    )
    one, two = P(KEYS_VIEW), P(KEYS_VIEW, None)
    placed = (
        P(), one, one, one, two, one, one, two, one, one, one, two, one, one, one, two, one,
    )
    return jax.shard_map(shards, mesh=split, in_specs=placed, out_specs=two, check_vma=False)
```

```python
import jax
import jax.numpy as jnp
from jax import lax
from jax.experimental import pallas as pl
from jax.experimental.pallas import tpu as pltpu
from jax.sharding import Mesh
from jax.sharding import PartitionSpec as P


KEYS_DEV = 512
GROUPS_DEV = 32
GROUPS = 4096
DELTA_DEV = 1024
A_DEV = 4096
D = 256
OWNERS = 32
CAP = 64
BLOCK = CAP + 8
KEYS = ("keys_0", "keys_1", "keys_2")
KEYS_VIEW = ("keys_0", "keys_1", "keys_2", "view")
F32, BF16, I32 = jnp.float32, jnp.bfloat16, jnp.int32
NN = (((1,), (0,)), ((), ()))
NT = (((1,), (1,)), ((), ()))
TN = (((0,), (0,)), ((), ()))
VMEM = pl.BlockSpec(memory_space=pltpu.VMEM)
SMEM = pl.BlockSpec(memory_space=pltpu.SMEM)


def dot(x, y, dims=NN):
    return lax.dot_general(x, y, dims, preferred_element_type=F32)


def rows_of(shape):
    return lax.broadcasted_iota(I32, shape, 0)


def lanes_of(shape):
    return lax.broadcasted_iota(I32, shape, 1)


def flat(x):
    return jnp.concatenate([x[j : j + 1, :] for j in range(x.shape[0])], axis=1)


def pick(condition, value):
    return jnp.where(condition, value, 0.0).astype(BF16)


def pack_kernel(with_group, me_ref, count_ref, table_ref, key_ref, mult_ref, *rest):
    group_ref = rest[0] if with_group else None
    payload_ref, out_ref = rest[-2:]
    rows = DELTA_DEV
    key = flat(key_ref[...])
    key_hi, key_lo = key >> 7, key & 127
    low = pick(rows_of((128, rows)) == key_lo, 1.0)
    table = table_ref[...]
    found = dot((table >> 7).astype(F32).astype(BF16), low) * 128.0 + dot(
        (table & 127).astype(F32).astype(BF16), low
    )
    slot = jnp.sum(jnp.where(rows_of((128, rows)) == key_hi, found, 0.0), axis=0, keepdims=True)
    slot = slot.astype(I32)
    owner, local = slot >> 9, slot & 511
    live = lanes_of((1, rows)) < count_ref[0]
    owner = jnp.where(live, owner, -1)
    marks = jnp.where(rows_of((OWNERS, rows)) == owner, 1.0, 0.0)
    step = jnp.where(
        (rows_of((128, 256)) < lanes_of((128, 256))) | (lanes_of((128, 256)) >= 128), 1.0, 0.0
    ).astype(BF16)
    before, carry = [], jnp.zeros((OWNERS, 128), F32)
    for j in range(rows // 128):
        counted = dot(marks[:, 128 * j : 128 * (j + 1)].astype(BF16), step)
        before.append(counted[:, :128] + carry)
        carry = carry + counted[:, 128:]
    rank = jnp.sum(marks * jnp.concatenate(before, axis=1), axis=0, keepdims=True).astype(I32)
    position = jnp.where(live, owner * CAP + rank, -1)
    sign = flat(mult_ref[...]).astype(F32)
    payload = payload_ref[...]
    for c in range(OWNERS // 4):
        chosen = pick(rows_of((4 * CAP, rows)) + 4 * CAP * c == position, sign)
        packed = dot(chosen, payload).astype(BF16)
        for j in range(4):
            out_ref[pl.ds((4 * c + j) * BLOCK, CAP), :] = packed[CAP * j : CAP * (j + 1)]
    field = rows_of((8, rows))
    value = jnp.where(field == 0, local & 255, jnp.where(field == 1, local >> 8, 0))
    if with_group:
        group = flat(group_ref[...])
        value = jnp.where(field == 2, group & 255, jnp.where(field == 3, group >> 8, value))
    value = jnp.broadcast_to(value.astype(F32)[None], (OWNERS, 8, rows)).reshape(8 * OWNERS, rows)
    sent = pick((rows_of((8 * OWNERS, rows)) >> 3) == owner, value)
    place = pick(rows_of((4 * CAP, rows)) == rank + CAP * (me_ref[0] % 4), 1.0)
    fields = dot(sent, place, NT).astype(BF16)
    for k in range(OWNERS):
        out_ref[pl.ds(k * BLOCK + CAP, 8), :] = fields[8 * k : 8 * k + 8]


def pack(me, count, table, key, mult, group, payload):
    extra = [] if group is None else [group.reshape(8, 128)]
    return pl.pallas_call(
        lambda *refs: pack_kernel(group is not None, *refs),
        out_shape=jax.ShapeDtypeStruct((OWNERS * BLOCK, D), BF16),
        in_specs=[SMEM, SMEM] + [VMEM] * (4 + len(extra)),
        out_specs=VMEM,
        name="pack_a" if extra else "pack_b",
    )(me, count, table, key.reshape(8, 128), mult.reshape(8, 128), *extra, payload)


def fields_of(ref, c):
    total = ref[pl.ds(4 * c * BLOCK + CAP, 8), :].astype(F32)
    for j in range(1, 4):
        total = total + ref[pl.ds((4 * c + j) * BLOCK + CAP, 8), :].astype(F32)
    total = total.astype(I32)
    return total[0:1] + 256 * total[1:2], total[2:3] + 256 * total[3:4]


def payload_of(ref, c):
    return jnp.concatenate(
        [ref[pl.ds((4 * c + j) * BLOCK, CAP), :] for j in range(4)], axis=0
    )


def spread(total_ref, view, outs):
    for s in range(4):
        outs[s][...] = total_ref[pl.ds(((view + s) % 4) * 128, 128), :]


def sum_b_kernel(view_ref, slot_ref, weight_ref, payload_ref, *rest):
    outs, total_ref = rest[:4], rest[4]
    total_ref[...] = jnp.zeros_like(total_ref)
    for c in range(4):
        slot = flat(slot_ref[8 * c : 8 * c + 8, :])
        weight = flat(weight_ref[8 * c : 8 * c + 8, :]).astype(F32)
        chosen = pick(rows_of((KEYS_DEV, 1024)) == slot, weight)
        total_ref[...] += dot(chosen, payload_ref[1024 * c : 1024 * (c + 1), :])
    spread(total_ref, view_ref[0], outs)


def sum_db_kernel(view_ref, in_ref, *rest):
    outs, total_ref = rest[:4], rest[4]
    total_ref[...] = jnp.zeros_like(total_ref)
    for c in range(8):
        slot, _ = fields_of(in_ref, c)
        chosen = pick(rows_of((KEYS_DEV, 256)) == slot, 1.0)
        total_ref[...] += dot(chosen, payload_of(in_ref, c))
    spread(total_ref, view_ref[0], outs)


def slices(kernel, view, *args):
    return pl.pallas_call(
        kernel,
        out_shape=[jax.ShapeDtypeStruct((128, D), F32)] * 4,
        in_specs=[SMEM] + [VMEM] * len(args),
        out_specs=[VMEM] * 4,
        scratch_shapes=[pltpu.VMEM((KEYS_DEV, D), F32)],
    )(view, *args)


def shift(x, s):
    return lax.ppermute(x, "view", [(j, (j + s) % 4) for j in range(4)])


def own_total(parts):
    got = [parts[0]] + [shift(parts[s], s) for s in (1, 2, 3)]
    return (got[0] + got[1]) + (got[2] + got[3])


def everyone(x):
    return [x] + [shift(x, s) for s in (1, 2, 3)]


def terms_of(ref, slot, weight, payload):
    chosen = pick(rows_of((KEYS_DEV, 256)) == slot, weight)
    got = dot(chosen, ref[...], TN)
    return (payload.astype(F32) * (got[:, :D] + got[:, D:])).astype(BF16)


def fill(ref, view, pieces):
    for s in range(4):
        at = pl.ds(((view + 4 - s) % 4) * 128, 128)
        value = pieces(s)
        high = value.astype(BF16)
        ref[at, :D] = high
        ref[at, D:] = (value - high.astype(F32)).astype(BF16)


def half_row(group, core):
    row = ((group >> 8) << 7) | (group & 127)
    return jnp.where(((group >> 7) & 1) == core, row, -1)


def half_sum(pieces, out_ref):
    def block(g, carry):
        total = None
        for at, terms in pieces:
            chosen = pick(rows_of((256, at.shape[1])) + 256 * g == at[...], 1.0)
            part = dot(chosen, terms[...])
            total = part if total is None else total + part
        out_ref[pl.ds(256 * g, 256), :] = total
        return carry

    lax.fori_loop(0, GROUPS // 512, block, 0)


def join_a_kernel(view_ref, *refs):
    db, (slot_ref, weight_ref, payload_ref), (out_ref, table_ref) = refs[:4], refs[4:7], refs[7:]
    fill(table_ref, view_ref[0], lambda s: db[s][...])
    for c in range(16):
        slot = flat(slot_ref[2 * c : 2 * c + 2, :])
        weight = flat(weight_ref[2 * c : 2 * c + 2, :]).astype(F32)
        at = pl.ds(256 * c, 256)
        out_ref[at, :] = terms_of(table_ref, slot, weight, payload_ref[at, :])


def join_d_kernel(view_ref, core_ref, *refs):
    db, b, (group_ref, in_ref, a_ref) = refs[:4], refs[4:8], refs[8:11]
    peer_ref, term_ref, own_a_ref, own_d_ref, whole_ref, peer_a_ref, peer_d_ref = refs[11:]
    core = core_ref[0]
    fill(whole_ref, view_ref[0], lambda s: b[s][...] + db[s][...])
    for c in range(4):
        at = pl.ds(1024 * c, 1024)
        group = flat(group_ref[8 * c : 8 * c + 8, :])
        own_a_ref[:, at] = half_row(group, core)
        peer_a_ref[:, at] = half_row(group, 1 - core)
    for c in range(8):
        slot, group = fields_of(in_ref, c)
        at = pl.ds(256 * c, 256)
        own_d_ref[:, at] = half_row(group, core)
        peer_d_ref[:, at] = half_row(group, 1 - core)
        term_ref[at, :] = terms_of(whole_ref, slot, 1.0, payload_of(in_ref, c))
    half_sum(((peer_a_ref, a_ref), (peer_d_ref, term_ref)), peer_ref)


def own_kernel(own_a_ref, a_ref, own_d_ref, d_ref, out_ref):
    half_sum(((own_a_ref, a_ref), (own_d_ref, d_ref)), out_ref)


def join(view, core, db, b, slot, group, weight, payload, received):
    rows = OWNERS * CAP
    table = pltpu.VMEM((KEYS_DEV, 2 * D), BF16)
    half = jax.ShapeDtypeStruct((GROUPS // 2, D), F32)
    a_terms = pl.pallas_call(
        join_a_kernel,
        out_shape=jax.ShapeDtypeStruct((A_DEV, D), BF16),
        in_specs=[SMEM] + [VMEM] * 7,
        out_specs=VMEM,
        scratch_shapes=[table],
        name="join_a",
    )(view, *db, slot.reshape(32, 128), weight.reshape(32, 128), payload)
    peer, d_terms, own_a, own_d = pl.pallas_call(
        join_d_kernel,
        out_shape=[
            half,
            jax.ShapeDtypeStruct((rows, D), BF16),
            jax.ShapeDtypeStruct((1, A_DEV), I32),
            jax.ShapeDtypeStruct((1, rows), I32),
        ],
        in_specs=[SMEM] * 2 + [VMEM] * 11,
        out_specs=[VMEM] * 4,
        scratch_shapes=[table, pltpu.VMEM((1, A_DEV), I32), pltpu.VMEM((1, rows), I32)],
        name="join_d",
    )(view, core, *db, *b, group.reshape(32, 128), received, a_terms)
    other = lax.ppermute(peer, "keys_2", [(0, 1), (1, 0)])
    own = pl.pallas_call(
        own_kernel, out_shape=half, in_specs=[VMEM] * 4, out_specs=VMEM, name="join_own"
    )(own_a, a_terms, own_d, d_terms)
    return (own + other).astype(BF16)


def exchange(packed):
    blocks = packed.reshape(OWNERS, BLOCK, D)
    return lax.all_to_all(blocks, KEYS, 0, 0, tiled=True).reshape(OWNERS * BLOCK, D)


def shards(
    key_slot,
    a_slot,
    a_group,
    a_weight,
    a_payload,
    b_slot,
    b_weight,
    b_payload,
    da_key,
    da_group,
    da_mult,
    da_payload,
    da_count,
    db_key,
    db_mult,
    db_payload,
    db_count,
):
    me = lax.axis_index(KEYS).astype(I32).reshape(1)
    view = lax.axis_index("view").astype(I32).reshape(1)
    table = key_slot.reshape(128, 128)
    core = lax.axis_index("keys_2").astype(I32).reshape(1)
    db_out = pack(me, db_count, table, db_key, db_mult, None, db_payload)
    da_out = pack(me, da_count, table, da_key, da_mult, da_group, da_payload)
    db_in = exchange(db_out)
    da_in = exchange(da_out)
    b_parts = slices(
        sum_b_kernel, view, b_slot.reshape(32, 128), b_weight.reshape(32, 128), b_payload
    )
    b = everyone(own_total(b_parts))
    db = everyone(own_total(slices(sum_db_kernel, view, db_in)))
    partial = join(view, core, db, b, a_slot, a_group, a_weight, a_payload, da_in)
    blocks = partial.reshape(GROUPS // 2 // GROUPS_DEV, GROUPS_DEV, D)
    blocks = lax.all_to_all(blocks, ("keys_0", "keys_1", "view"), 0, 0, tiled=True)
    return jnp.sum(blocks.astype(F32), axis=0)


def solution(mesh):
    split = Mesh(
        mesh.devices.reshape(4, 4, 2, mesh.shape["view"]), ("keys_0", "keys_1", "keys_2", "view")
    )
    one, two = P(KEYS_VIEW), P(KEYS_VIEW, None)
    placed = (
        P(), one, one, one, two, one, one, two, one, one, one, two, one, one, one, two, one,
    )
    return jax.shard_map(shards, mesh=split, in_specs=placed, out_specs=two, check_vma=False)
```

```python
import jax
import jax.numpy as jnp
from jax import lax
from jax.experimental import pallas as pl
from jax.experimental.pallas import tpu as pltpu
from jax.sharding import Mesh
from jax.sharding import PartitionSpec as P


KEYS_DEV = 512
GROUPS_DEV = 32
GROUPS = 4096
DELTA_DEV = 1024
A_DEV = 4096
D = 256
OWNERS = 32
CAP = 64
BLOCK = CAP + 8
SORT, SORT_RUNS = 1024, 2
WINDOW = 1408
LIMIT = pltpu.CompilerParams(vmem_limit_bytes=16 * 2**20)
KEYS = ("keys_0", "keys_1", "keys_2")
KEYS_VIEW = ("keys_0", "keys_1", "keys_2", "view")
F32, BF16, I32, I16 = jnp.float32, jnp.bfloat16, jnp.int32, jnp.int16
NN = (((1,), (0,)), ((), ()))
NT = (((1,), (1,)), ((), ()))
TN = (((0,), (0,)), ((), ()))
VMEM = pl.BlockSpec(memory_space=pltpu.VMEM)
SMEM = pl.BlockSpec(memory_space=pltpu.SMEM)


def dot(x, y, dims=NN):
    return lax.dot_general(x, y, dims, preferred_element_type=F32)


def rows_of(shape):
    return lax.broadcasted_iota(I32, shape, 0)


def lanes_of(shape):
    return lax.broadcasted_iota(I32, shape, 1)


def flat(x):
    return jnp.concatenate([x[j : j + 1, :] for j in range(x.shape[0])], axis=1)


def pick(condition, value):
    return jnp.where(condition, value, 0.0).astype(BF16)


def onehot(rows, index, value=None):
    hit = lax.broadcasted_iota(I16, (rows, index.shape[1]), 0) == index.astype(I16)
    one = jnp.ones((), BF16) if value is None else value.astype(BF16)
    return jnp.where(hit, one, jnp.zeros((), BF16))


def counted_before(marks):
    step = jnp.where(
        (rows_of((128, 256)) < lanes_of((128, 256))) | (lanes_of((128, 256)) >= 128), 1.0, 0.0
    ).astype(BF16)
    before, carry = [], jnp.zeros((marks.shape[0], 128), F32)
    for j in range(marks.shape[1] // 128):
        counted = dot(marks[:, 128 * j : 128 * (j + 1)].astype(BF16), step)
        before.append(counted[:, :128] + carry)
        carry = carry + counted[:, 128:]
    return jnp.concatenate(before, axis=1)


def pack_kernel(with_group, me_ref, count_ref, table_ref, key_ref, mult_ref, *rest):
    group_ref = rest[0] if with_group else None
    payload_ref, out_ref = rest[-2:]
    rows = DELTA_DEV
    key = flat(key_ref[...])
    key_hi, key_lo = key >> 7, key & 127
    low = onehot(128, key_lo)
    table = table_ref[...]
    found = dot((table >> 7).astype(F32).astype(BF16), low) * 128.0 + dot(
        (table & 127).astype(F32).astype(BF16), low
    )
    slot = jnp.sum(jnp.where(rows_of((128, rows)) == key_hi, found, 0.0), axis=0, keepdims=True)
    slot = slot.astype(I32)
    owner, local = slot >> 9, slot & 511
    live = lanes_of((1, rows)) < count_ref[0]
    owner = jnp.where(live, owner, -1)
    marks = jnp.where(rows_of((OWNERS, rows)) == owner, 1.0, 0.0)
    rank = jnp.sum(marks * counted_before(marks), axis=0, keepdims=True).astype(I32)
    position = jnp.where(live, owner * CAP + rank, -1)
    sign = flat(mult_ref[...]).astype(F32)
    payload = payload_ref[...]
    for c in range(OWNERS // 4):
        chosen = onehot(4 * CAP, position - 4 * CAP * c, sign)
        packed = dot(chosen, payload).astype(BF16)
        for j in range(4):
            out_ref[pl.ds((4 * c + j) * BLOCK, CAP), :] = packed[CAP * j : CAP * (j + 1)]
    field = rows_of((8, rows))
    value = jnp.where(field == 0, local & 255, jnp.where(field == 1, local >> 8, 0))
    if with_group:
        group = flat(group_ref[...])
        value = jnp.where(field == 2, group & 255, jnp.where(field == 3, group >> 8, value))
    value = jnp.broadcast_to(value.astype(F32)[None], (OWNERS, 8, rows)).reshape(8 * OWNERS, rows)
    sent = pick((rows_of((8 * OWNERS, rows)) >> 3) == owner, value)
    place = onehot(4 * CAP, rank + CAP * (me_ref[0] % 4))
    fields = dot(sent, place, NT).astype(BF16)
    for k in range(OWNERS):
        out_ref[pl.ds(k * BLOCK + CAP, 8), :] = fields[8 * k : 8 * k + 8]


def pack(me, count, table, key, mult, group, payload):
    extra = [] if group is None else [group.reshape(8, 128)]
    return pl.pallas_call(
        lambda *refs: pack_kernel(group is not None, *refs),
        out_shape=jax.ShapeDtypeStruct((OWNERS * BLOCK, D), BF16),
        in_specs=[SMEM, SMEM] + [VMEM] * (4 + len(extra)),
        out_specs=VMEM,
        compiler_params=LIMIT,
        name="pack_a" if extra else "pack_b",
    )(me, count, table, key.reshape(8, 128), mult.reshape(8, 128), *extra, payload)


def fields_of(ref, c):
    total = ref[pl.ds(4 * c * BLOCK + CAP, 8), :].astype(F32)
    for j in range(1, 4):
        total = total + ref[pl.ds((4 * c + j) * BLOCK + CAP, 8), :].astype(F32)
    total = total.astype(I32)
    return total[0:1] + 256 * total[1:2], total[2:3] + 256 * total[3:4]


def payload_of(ref, c):
    return jnp.concatenate(
        [ref[pl.ds((4 * c + j) * BLOCK, CAP), :] for j in range(4)], axis=0
    )


def spread(total_ref, view, outs):
    for s in range(4):
        outs[s][...] = total_ref[pl.ds(((view + s) % 4) * 128, 128), :]


def sum_b_kernel(view_ref, slot_ref, weight_ref, payload_ref, *rest):
    outs, total_ref = rest[:4], rest[4]
    total_ref[...] = jnp.zeros_like(total_ref)
    for c in range(4):
        slot = flat(slot_ref[8 * c : 8 * c + 8, :])
        weight = flat(weight_ref[8 * c : 8 * c + 8, :]).astype(F32)
        chosen = onehot(KEYS_DEV, slot, weight)
        total_ref[...] += dot(chosen, payload_ref[1024 * c : 1024 * (c + 1), :])
    spread(total_ref, view_ref[0], outs)


def sum_db_kernel(view_ref, in_ref, *rest):
    outs, total_ref = rest[:4], rest[4]
    total_ref[...] = jnp.zeros_like(total_ref)
    for c in range(8):
        slot, _ = fields_of(in_ref, c)
        chosen = onehot(KEYS_DEV, slot)
        total_ref[...] += dot(chosen, payload_of(in_ref, c))
    spread(total_ref, view_ref[0], outs)


def slices(kernel, view, *args):
    return pl.pallas_call(
        kernel,
        out_shape=[jax.ShapeDtypeStruct((128, D), F32)] * 4,
        in_specs=[SMEM] + [VMEM] * len(args),
        out_specs=[VMEM] * 4,
        scratch_shapes=[pltpu.VMEM((KEYS_DEV, D), F32)],
        compiler_params=LIMIT,
    )(view, *args)


def shift(x, s):
    return lax.ppermute(x, "view", [(j, (j + s) % 4) for j in range(4)])


def own_total(parts):
    got = [parts[0]] + [shift(parts[s], s) for s in (1, 2, 3)]
    return (got[0] + got[1]) + (got[2] + got[3])


def everyone(x):
    return [x] + [shift(x, s) for s in (1, 2, 3)]


def fill(ref, view, pieces):
    for s in range(4):
        at = pl.ds(((view + 4 - s) % 4) * 128, 128)
        value = pieces(s)
        high = value.astype(BF16)
        ref[at, :D] = high
        ref[at, D:] = (value - high.astype(F32)).astype(BF16)


def terms_of(ref, slot, weight, payload):
    got = dot(onehot(KEYS_DEV, slot, weight), ref[...], TN)
    return (payload.astype(F32) * (got[:, :D] + got[:, D:])).astype(BF16)


def place_of(group, core):
    own = jnp.where(((group >> 7) & 1) == core, GROUPS // 2, 0)
    return own + ((group >> 8) << 7) + (group & 127)


def sort_kernel(core_ref, slot_ref, group_ref, weight_ref, payload_ref, out_ref, slots_ref, places_ref, weights_ref):
    for s in range(SORT_RUNS):
        rows = slice(8 * s, 8 * s + 8)
        slot, weight = flat(slot_ref[rows, :]), flat(weight_ref[rows, :])
        place = place_of(flat(group_ref[rows, :]), core_ref[0])
        bucket = place >> 6
        shape = (GROUPS // 64, SORT)
        marks = jnp.where(rows_of(shape) == bucket, 1.0, 0.0)
        first = jnp.sum(jnp.where(bucket < rows_of(shape), 1.0, 0.0), axis=1, keepdims=True)
        position = jnp.sum(marks * (counted_before(marks) + first), axis=0, keepdims=True)
        order = onehot(SORT, position.astype(I32))
        moved = dot(order, payload_ref[SORT * s : SORT * (s + 1), :]).astype(BF16)
        value, field = jnp.zeros((8, SORT), I32), rows_of((8, SORT))
        for q, part in enumerate((slot & 255, slot >> 8, weight, place & 255, place >> 8)):
            value = jnp.where(field == q, part, value)
        fields = dot(value.astype(F32).astype(BF16), order, NT).astype(I32)
        for j in range(4):
            at = slice(512 * j + 256 * s, 512 * j + 256 * (s + 1))
            part = slice(256 * j, 256 * (j + 1))
            out_ref[at, :] = moved[part]
            slots_ref[:, at] = fields[0:1, part] + 256 * fields[1:2, part]
            weights_ref[:, at] = fields[2:3, part]
            places_ref[:, at] = fields[3:4, part] + 256 * fields[4:5, part]


def sort(h, core, slot, group, weight, payload):
    rows = SORT_RUNS * SORT
    line = jax.ShapeDtypeStruct((1, rows), I32)
    return pl.pallas_call(
        sort_kernel,
        out_shape=[jax.ShapeDtypeStruct((rows, D), BF16), line, line, line],
        grid=(1,),
        in_specs=[SMEM] + [pl.BlockSpec((rows // 128, 128), lambda i: (h, 0))] * 3 + [pl.BlockSpec((rows, D), lambda i: (h, 0))],
        out_specs=[VMEM] * 4,
        compiler_params=LIMIT,
    )(core, slot.reshape(32, 128), group.reshape(32, 128), weight.reshape(32, 128), payload)


def join_kernel(view_ref, core_ref, *refs):
    db, b, sorted_rows, in_ref = refs[:4], refs[4:8], (refs[8:12], refs[12:16]), refs[16]
    peer_ref, own_ref, delta_ref, place_ref = refs[17:21]
    table_ref, whole_ref, term_ref, line_ref, total_ref = refs[21:]
    view, core = view_ref[0], core_ref[0]
    fill(table_ref, view, lambda s: db[s][...])
    fill(whole_ref, view, lambda s: b[s][...] + db[s][...])
    total_ref[...] = jnp.zeros_like(total_ref)
    starts, ends = [], []
    for j in range(4):
        for h, (payload_ref, slots_ref, places_ref, weights_ref) in enumerate(sorted_rows):
            part, at = slice(512 * j, 512 * (j + 1)), slice(1024 * j + 512 * h, 1024 * j + 512 * (h + 1))
            term_ref[at, :] = terms_of(table_ref, slots_ref[:, part], weights_ref[:, part].astype(F32), payload_ref[part, :])
            line_ref[:, at] = places_ref[:, part]
        line = line_ref[:, 1024 * j : 1024 * (j + 1)]
        starts.append(pl.multiple_of((jnp.min(line) >> 6) << 6, 64))
        ends.append(jnp.max(line))

    def window(j, start):
        rows = slice(1024 * j, 1024 * (j + 1))
        chosen = onehot(WINDOW, line_ref[:, rows] - start)
        total_ref[pl.ds(start, WINDOW), :] += dot(chosen, term_ref[rows, :])

    for j in range(4):
        window(j, starts[j])
    for j in range(4):
        def more(i, carry, j=j):
            window(j, pl.multiple_of(starts[j] + i * WINDOW, 64))
            return carry

        lax.fori_loop(1, (ends[j] - starts[j]) // WINDOW + 1, more, 0)
    for c in range(8):
        slot, group = fields_of(in_ref, c)
        at = slice(256 * c, 256 * (c + 1))
        place_ref[:, at] = place_of(group, core)
        delta_ref[at, :] = terms_of(whole_ref, slot, None, payload_of(in_ref, c))
    for g in range(GROUPS // 2 // 512):
        at = slice(512 * g, 512 * (g + 1))
        chosen = onehot(512, place_ref[...] - 512 * g)
        peer_ref[at, :] = total_ref[at, :] + dot(chosen, delta_ref[...])
    own_ref[...] = total_ref[GROUPS // 2 : GROUPS, :]


def own_kernel(own_ref, delta_ref, place_ref, out_ref):
    for g in range(GROUPS // 2 // 512):
        at = slice(512 * g, 512 * (g + 1))
        chosen = onehot(512, place_ref[...] - GROUPS // 2 - 512 * g)
        out_ref[at, :] = own_ref[at, :] + dot(chosen, delta_ref[...])


def join(view, core, db, b, halves, received):
    rows = OWNERS * CAP
    table = pltpu.VMEM((KEYS_DEV, 2 * D), BF16)
    half = jax.ShapeDtypeStruct((GROUPS // 2, D), F32)
    peer, own, delta, place = pl.pallas_call(
        join_kernel,
        out_shape=[
            half,
            half,
            jax.ShapeDtypeStruct((rows, D), BF16),
            jax.ShapeDtypeStruct((1, rows), I32),
        ],
        in_specs=[SMEM] * 2 + [VMEM] * 17,
        out_specs=[VMEM] * 4,
        scratch_shapes=[
            table,
            table,
            pltpu.VMEM((A_DEV, D), BF16),
            pltpu.VMEM((1, A_DEV), I32),
            pltpu.VMEM((GROUPS + WINDOW, D), F32),
        ],
        compiler_params=pltpu.CompilerParams(vmem_limit_bytes=36 * 2**20),
        name="join",
    )(view, core, *db, *b, *halves[0], *halves[1], received)
    other = lax.ppermute(peer, "keys_2", [(0, 1), (1, 0)])
    own = pl.pallas_call(
        own_kernel, out_shape=half, in_specs=[VMEM] * 3, out_specs=VMEM, name="join_own", compiler_params=LIMIT
    )(own, delta, place)
    return (own + other).astype(BF16)


def exchange(packed):
    blocks = packed.reshape(OWNERS, BLOCK, D)
    return lax.all_to_all(blocks, KEYS, 0, 0, tiled=True).reshape(OWNERS * BLOCK, D)


def shards(
    key_slot,
    a_slot,
    a_group,
    a_weight,
    a_payload,
    b_slot,
    b_weight,
    b_payload,
    da_key,
    da_group,
    da_mult,
    da_payload,
    da_count,
    db_key,
    db_mult,
    db_payload,
    db_count,
):
    me = lax.axis_index(KEYS).astype(I32).reshape(1)
    view = lax.axis_index("view").astype(I32).reshape(1)
    table = key_slot.reshape(128, 128)
    core = lax.axis_index("keys_2").astype(I32).reshape(1)
    db_out = pack(me, db_count, table, db_key, db_mult, None, db_payload)
    da_out = pack(me, da_count, table, da_key, da_mult, da_group, da_payload)
    db_in = exchange(db_out)
    da_in = exchange(da_out)
    b_parts = slices(
        sum_b_kernel, view, b_slot.reshape(32, 128), b_weight.reshape(32, 128), b_payload
    )
    b = everyone(own_total(b_parts))
    db = everyone(own_total(slices(sum_db_kernel, view, db_in)))
    halves = [sort(h, core, a_slot, a_group, a_weight, a_payload) for h in (0, 1)]
    partial = join(view, core, db, b, halves, da_in)
    blocks = partial.reshape(GROUPS // 2 // GROUPS_DEV, GROUPS_DEV, D)
    blocks = lax.all_to_all(blocks, ("keys_0", "keys_1", "view"), 0, 0, tiled=True)
    return jnp.sum(blocks.astype(F32), axis=0)


def solution(mesh):
    split = Mesh(
        mesh.devices.reshape(4, 4, 2, mesh.shape["view"]), ("keys_0", "keys_1", "keys_2", "view")
    )
    one, two = P(KEYS_VIEW), P(KEYS_VIEW, None)
    placed = (
        P(), one, one, one, two, one, one, two, one, one, one, two, one, one, one, two, one,
    )
    return jax.shard_map(shards, mesh=split, in_specs=placed, out_specs=two, check_vma=False)
```

```python
import jax
import jax.numpy as jnp
from jax import lax
from jax.experimental import pallas as pl
from jax.experimental.pallas import tpu as pltpu
from jax.sharding import Mesh
from jax.sharding import PartitionSpec as P


KEYS_DEV = 512
GROUPS_DEV = 32
GROUPS = 4096
DELTA_DEV = 1024
A_DEV = 4096
D = 256
OWNERS = 32
CAP = 64
BLOCK = CAP + 8
SORT, SORT_RUNS = 1024, 2
WINDOW = 1408
LIMIT = pltpu.CompilerParams(vmem_limit_bytes=16 * 2**20)
KEYS = ("keys_0", "keys_1", "keys_2")
KEYS_VIEW = ("keys_0", "keys_1", "keys_2", "view")
F32, BF16, I32, I16 = jnp.float32, jnp.bfloat16, jnp.int32, jnp.int16
NN = (((1,), (0,)), ((), ()))
NT = (((1,), (1,)), ((), ()))
TN = (((0,), (0,)), ((), ()))
VMEM = pl.BlockSpec(memory_space=pltpu.VMEM)
SMEM = pl.BlockSpec(memory_space=pltpu.SMEM)
HBM = pl.BlockSpec(memory_space=pltpu.HBM)


def in_hbm(x):
    return pltpu.with_memory_space_constraint(x, pltpu.HBM)


def dot(x, y, dims=NN):
    return lax.dot_general(x, y, dims, preferred_element_type=F32)


def rows_of(shape):
    return lax.broadcasted_iota(I32, shape, 0)


def lanes_of(shape):
    return lax.broadcasted_iota(I32, shape, 1)


def flat(x):
    return jnp.concatenate([x[j : j + 1, :] for j in range(x.shape[0])], axis=1)


def pick(condition, value):
    return jnp.where(condition, value, 0.0).astype(BF16)


def onehot(rows, index, value=None):
    hit = lax.broadcasted_iota(I16, (rows, index.shape[1]), 0) == index.astype(I16)
    one = jnp.ones((), BF16) if value is None else value.astype(BF16)
    return jnp.where(hit, one, jnp.zeros((), BF16))


def counted_before(marks):
    step = jnp.where(
        (rows_of((128, 256)) < lanes_of((128, 256))) | (lanes_of((128, 256)) >= 128), 1.0, 0.0
    ).astype(BF16)
    before, carry = [], jnp.zeros((marks.shape[0], 128), F32)
    for j in range(marks.shape[1] // 128):
        counted = dot(marks[:, 128 * j : 128 * (j + 1)].astype(BF16), step)
        before.append(counted[:, :128] + carry)
        carry = carry + counted[:, 128:]
    return jnp.concatenate(before, axis=1)


def pack_kernel(with_group, me_ref, count_ref, table_ref, key_ref, mult_ref, *rest):
    group_ref = rest[0] if with_group else None
    payload_ref, out_ref = rest[-2:]
    rows = DELTA_DEV
    key = flat(key_ref[...])
    key_hi, key_lo = key >> 7, key & 127
    low = onehot(128, key_lo)
    table = table_ref[...]
    found = dot((table >> 7).astype(F32).astype(BF16), low) * 128.0 + dot(
        (table & 127).astype(F32).astype(BF16), low
    )
    slot = jnp.sum(jnp.where(rows_of((128, rows)) == key_hi, found, 0.0), axis=0, keepdims=True)
    slot = slot.astype(I32)
    owner, local = slot >> 9, slot & 511
    live = lanes_of((1, rows)) < count_ref[0]
    owner = jnp.where(live, owner, -1)
    marks = jnp.where(rows_of((OWNERS, rows)) == owner, 1.0, 0.0)
    rank = jnp.sum(marks * counted_before(marks), axis=0, keepdims=True).astype(I32)
    position = jnp.where(live, owner * CAP + rank, -1)
    sign = flat(mult_ref[...]).astype(F32)
    payload = payload_ref[...]
    for c in range(OWNERS // 4):
        chosen = onehot(4 * CAP, position - 4 * CAP * c, sign)
        packed = dot(chosen, payload).astype(BF16)
        for j in range(4):
            out_ref[pl.ds((4 * c + j) * BLOCK, CAP), :] = packed[CAP * j : CAP * (j + 1)]
    field = rows_of((8, rows))
    value = jnp.where(field == 0, local & 255, jnp.where(field == 1, local >> 8, 0))
    if with_group:
        group = flat(group_ref[...])
        value = jnp.where(field == 2, group & 255, jnp.where(field == 3, group >> 8, value))
    value = jnp.broadcast_to(value.astype(F32)[None], (OWNERS, 8, rows)).reshape(8 * OWNERS, rows)
    sent = pick((rows_of((8 * OWNERS, rows)) >> 3) == owner, value)
    place = onehot(4 * CAP, rank + CAP * (me_ref[0] % 4))
    fields = dot(sent, place, NT).astype(BF16)
    for k in range(OWNERS):
        out_ref[pl.ds(k * BLOCK + CAP, 8), :] = fields[8 * k : 8 * k + 8]


def pack(me, count, table, key, mult, group, payload):
    extra = [] if group is None else [group.reshape(8, 128)]
    return pl.pallas_call(
        lambda *refs: pack_kernel(group is not None, *refs),
        out_shape=pltpu.HBM((OWNERS * BLOCK, D), BF16),
        in_specs=[SMEM, SMEM] + [VMEM] * (4 + len(extra)),
        out_specs=VMEM,
        compiler_params=LIMIT,
        name="pack_a" if extra else "pack_b",
    )(me, count, *map(in_hbm, (table, key.reshape(8, 128), mult.reshape(8, 128), *extra, payload)))


def fields_of(ref, c):
    total = ref[pl.ds(4 * c * BLOCK + CAP, 8), :].astype(F32)
    for j in range(1, 4):
        total = total + ref[pl.ds((4 * c + j) * BLOCK + CAP, 8), :].astype(F32)
    total = total.astype(I32)
    return total[0:1] + 256 * total[1:2], total[2:3] + 256 * total[3:4]


def payload_of(ref, c):
    return jnp.concatenate(
        [ref[pl.ds((4 * c + j) * BLOCK, CAP), :] for j in range(4)], axis=0
    )


def spread(total_ref, view, outs):
    for s in range(4):
        outs[s][...] = total_ref[pl.ds(((view + s) % 4) * 128, 128), :]


def sum_b_kernel(view_ref, slot_ref, weight_ref, payload_ref, *rest):
    outs, total_ref = rest[:4], rest[4]
    total_ref[...] = jnp.zeros_like(total_ref)
    for c in range(4):
        slot = flat(slot_ref[8 * c : 8 * c + 8, :])
        weight = flat(weight_ref[8 * c : 8 * c + 8, :]).astype(F32)
        chosen = onehot(KEYS_DEV, slot, weight)
        total_ref[...] += dot(chosen, payload_ref[1024 * c : 1024 * (c + 1), :])
    spread(total_ref, view_ref[0], outs)


def sum_db_kernel(view_ref, in_ref, *rest):
    outs, total_ref = rest[:4], rest[4]
    total_ref[...] = jnp.zeros_like(total_ref)
    for c in range(8):
        slot, _ = fields_of(in_ref, c)
        chosen = onehot(KEYS_DEV, slot)
        total_ref[...] += dot(chosen, payload_of(in_ref, c))
    spread(total_ref, view_ref[0], outs)


def slices(kernel, view, *args):
    return pl.pallas_call(
        kernel,
        out_shape=[jax.ShapeDtypeStruct((128, D), F32)] * 4,
        in_specs=[SMEM] + [VMEM] * len(args),
        out_specs=[VMEM] * 4,
        scratch_shapes=[pltpu.VMEM((KEYS_DEV, D), F32)],
        compiler_params=LIMIT,
    )(view, *args)


def shift(x, s):
    return lax.ppermute(x, "view", [(j, (j + s) % 4) for j in range(4)])


def own_total(parts):
    got = [parts[0]] + [shift(parts[s], s) for s in (1, 2, 3)]
    return (got[0] + got[1]) + (got[2] + got[3])


def everyone(x):
    return [x] + [shift(x, s) for s in (1, 2, 3)]


def fill(ref, view, pieces):
    for s in range(4):
        at = pl.ds(((view + 4 - s) % 4) * 128, 128)
        value = pieces(s)
        high = value.astype(BF16)
        ref[at, :D] = high
        ref[at, D:] = (value - high.astype(F32)).astype(BF16)


def terms_of(ref, slot, weight, payload):
    got = dot(onehot(KEYS_DEV, slot, weight), ref[...], TN)
    return (payload.astype(F32) * (got[:, :D] + got[:, D:])).astype(BF16)


def place_of(group, core):
    own = jnp.where(((group >> 7) & 1) == core, GROUPS // 2, 0)
    return own + ((group >> 8) << 7) + (group & 127)


def sort_kernel(core_ref, slot_ref, group_ref, weight_ref, payload_ref, out_ref, field_ref):
    for s in range(SORT_RUNS):
        rows = slice(8 * s, 8 * s + 8)
        slot, weight = flat(slot_ref[rows, :]), flat(weight_ref[rows, :])
        place = place_of(flat(group_ref[rows, :]), core_ref[0])
        bucket = place >> 6
        shape = (GROUPS // 64, SORT)
        marks = jnp.where(rows_of(shape) == bucket, 1.0, 0.0)
        first = jnp.sum(jnp.where(bucket < rows_of(shape), 1.0, 0.0), axis=1, keepdims=True)
        position = jnp.sum(marks * (counted_before(marks) + first), axis=0, keepdims=True)
        order = onehot(SORT, position.astype(I32))
        moved = dot(order, payload_ref[SORT * s : SORT * (s + 1), :]).astype(BF16)
        value, field = jnp.zeros((8, SORT), I32), rows_of((8, SORT))
        for q, part in enumerate((slot & 255, slot >> 8, weight, place & 255, place >> 8)):
            value = jnp.where(field == q, part, value)
        fields = dot(value.astype(F32).astype(BF16), order, NT).astype(I32)
        for j in range(4):
            at = slice(512 * j + 256 * s, 512 * j + 256 * (s + 1))
            part = slice(256 * j, 256 * (j + 1))
            out_ref[at, :] = moved[part]
            field_ref[:, at] = fields[:, part]


def sort(h, core, slot, group, weight, payload):
    rows = SORT_RUNS * SORT
    return pl.pallas_call(
        sort_kernel,
        out_shape=[pltpu.HBM((rows, D), BF16), pltpu.HBM((8, rows), I32)],
        grid=(1,),
        in_specs=[SMEM] + [pl.BlockSpec((rows // 128, 128), lambda i: (h, 0))] * 3 + [pl.BlockSpec((rows, D), lambda i: (h, 0))],
        out_specs=[VMEM] * 2,
        compiler_params=LIMIT,
    )(core, slot.reshape(32, 128), group.reshape(32, 128), weight.reshape(32, 128), payload)


def join_kernel(view_ref, core_ref, *refs):
    db, b, (first, second, fields0, fields1, in_ref) = refs[:4], refs[4:8], refs[8:13]
    peer_ref, own_ref, delta_ref, place_ref = refs[13:17]
    table_ref, whole_ref, sorted_ref, field_ref, line_ref, total_ref, sems = refs[17:]
    copies = [
        pltpu.make_async_copy(source, target, sems.at[n])
        for n, (source, target) in enumerate(
            (
                (fields0, field_ref.at[0]),
                (fields1, field_ref.at[1]),
                (first, sorted_ref.at[0]),
                (second, sorted_ref.at[1]),
            )
        )
    ]
    for copy in copies:
        copy.start()
    view, core = view_ref[0], core_ref[0]
    fill(table_ref, view, lambda s: db[s][...])
    fill(whole_ref, view, lambda s: b[s][...] + db[s][...])
    for c in range(8):
        slot, group = fields_of(in_ref, c)
        at = slice(256 * c, 256 * (c + 1))
        place_ref[:, at] = place_of(group, core)
        delta_ref[at, :] = terms_of(whole_ref, slot, None, payload_of(in_ref, c))
    for g in range(GROUPS // 2 // 512):
        chosen = onehot(512, place_ref[...] - 512 * g)
        total_ref[512 * g : 512 * (g + 1), :] = dot(chosen, delta_ref[...])
    total_ref[GROUPS // 2 :, :] = jnp.zeros((GROUPS // 2 + WINDOW, D), F32)
    for copy in copies:
        copy.wait()
    starts, ends = [], []
    for j in range(4):
        for h in range(2):
            part, at = slice(512 * j, 512 * (j + 1)), slice(512 * h, 512 * (h + 1))
            fields = field_ref[h, :, part]
            slot = fields[0:1] + 256 * fields[1:2]
            sorted_ref[h, part, :] = terms_of(table_ref, slot, fields[2:3].astype(F32), sorted_ref[h, part, :])
            line_ref[j : j + 1, at] = fields[3:4] + 256 * fields[4:5]
        line = line_ref[j : j + 1, :]
        starts.append(pl.multiple_of((jnp.min(line) >> 6) << 6, 64))
        ends.append(jnp.max(line))

    def window(j, start):
        chosen = onehot(WINDOW, line_ref[j : j + 1, :] - start)
        rows = sorted_ref[:, 512 * j : 512 * (j + 1), :].reshape(1024, D)
        total_ref[pl.ds(start, WINDOW), :] += dot(chosen, rows)

    for j in range(4):
        window(j, starts[j])
    for j in range(4):
        def more(i, carry, j=j):
            window(j, pl.multiple_of(starts[j] + i * WINDOW, 64))
            return carry

        lax.fori_loop(1, (ends[j] - starts[j]) // WINDOW + 1, more, 0)
    peer_ref[...] = total_ref[: GROUPS // 2, :]
    own_ref[...] = total_ref[GROUPS // 2 : GROUPS, :]


def own_kernel(own_ref, delta_ref, place_ref, out_ref):
    for g in range(GROUPS // 2 // 512):
        at = slice(512 * g, 512 * (g + 1))
        chosen = onehot(512, place_ref[...] - GROUPS // 2 - 512 * g)
        out_ref[at, :] = own_ref[at, :] + dot(chosen, delta_ref[...])


def join(view, core, db, b, halves, received):
    rows = OWNERS * CAP
    table = pltpu.VMEM((KEYS_DEV, 2 * D), BF16)
    half = jax.ShapeDtypeStruct((GROUPS // 2, D), F32)
    peer, own, delta, place = pl.pallas_call(
        join_kernel,
        out_shape=[
            half,
            half,
            jax.ShapeDtypeStruct((rows, D), BF16),
            jax.ShapeDtypeStruct((1, rows), I32),
        ],
        in_specs=[SMEM] * 2 + [VMEM] * 8 + [HBM] * 4 + [VMEM],
        out_specs=[VMEM] * 4,
        scratch_shapes=[
            table,
            table,
            pltpu.VMEM((2, A_DEV // 2, D), BF16),
            pltpu.VMEM((2, 8, A_DEV // 2), I32),
            pltpu.VMEM((4, 1024), I32),
            pltpu.VMEM((GROUPS + WINDOW, D), F32),
            pltpu.SemaphoreType.DMA((4,)),
        ],
        compiler_params=pltpu.CompilerParams(vmem_limit_bytes=32 * 2**20),
        name="join",
    )(view, core, *db, *b, *(in_hbm(half[i]) for i in (0, 1) for half in halves), received)
    other = lax.ppermute(peer, "keys_2", [(0, 1), (1, 0)])
    own = pl.pallas_call(
        own_kernel, out_shape=half, in_specs=[VMEM] * 3, out_specs=VMEM, name="join_own", compiler_params=LIMIT
    )(own, delta, place)
    return (own + other).astype(BF16)


def exchange(packed):
    blocks = packed.reshape(OWNERS, BLOCK, D)
    return lax.all_to_all(blocks, KEYS, 0, 0, tiled=True).reshape(OWNERS * BLOCK, D)


def shards(
    key_slot,
    a_slot,
    a_group,
    a_weight,
    a_payload,
    b_slot,
    b_weight,
    b_payload,
    da_key,
    da_group,
    da_mult,
    da_payload,
    da_count,
    db_key,
    db_mult,
    db_payload,
    db_count,
):
    me = lax.axis_index(KEYS).astype(I32).reshape(1)
    view = lax.axis_index("view").astype(I32).reshape(1)
    table = key_slot.reshape(128, 128)
    core = lax.axis_index("keys_2").astype(I32).reshape(1)
    db_out = pack(me, db_count, table, db_key, db_mult, None, db_payload)
    da_out = pack(me, da_count, table, da_key, da_mult, da_group, da_payload)
    db_in = in_hbm(exchange(db_out))
    da_in = exchange(da_out)
    b_parts = slices(
        sum_b_kernel, view, b_slot.reshape(32, 128), b_weight.reshape(32, 128), b_payload
    )
    b = everyone(own_total(b_parts))
    db = everyone(own_total(slices(sum_db_kernel, view, db_in)))
    halves = [sort(h, core, a_slot, a_group, a_weight, a_payload) for h in (0, 1)]
    partial = join(view, core, db, b, halves, da_in)
    blocks = partial.reshape(GROUPS // 2 // GROUPS_DEV, GROUPS_DEV, D)
    blocks = lax.all_to_all(blocks, ("keys_0", "keys_1", "view"), 0, 0, tiled=True)
    return jnp.sum(blocks.astype(F32), axis=0)


def solution(mesh):
    split = Mesh(
        mesh.devices.reshape(4, 4, 2, mesh.shape["view"]), ("keys_0", "keys_1", "keys_2", "view")
    )
    one, two = P(KEYS_VIEW), P(KEYS_VIEW, None)
    placed = (
        P(), one, one, one, two, one, one, two, one, one, one, two, one, one, one, two, one,
    )
    return jax.shard_map(shards, mesh=split, in_specs=placed, out_specs=two, check_vma=False)
```

```python
import functools

import jax
import jax.numpy as jnp
from jax import lax
from jax.experimental import pallas as pl
from jax.experimental.pallas import tpu as pltpu
from jax.sharding import Mesh
from jax.sharding import PartitionSpec as P


KEYS_DEV = 512
GROUPS_DEV = 32
GROUPS = 4096
DELTA_DEV = 1024
A_DEV = 4096
D = 256
OWNERS = 32
CAP = 64
BLOCK = CAP + 8
SORT, SORT_RUNS = 1024, 2
WINDOW = 1408
STEP = 256
LIMIT = pltpu.CompilerParams(vmem_limit_bytes=16 * 2**20)
KEYS = ("keys_0", "keys_1", "keys_2")
KEYS_VIEW = ("keys_0", "keys_1", "keys_2", "view")
F32, BF16, I32, I16 = jnp.float32, jnp.bfloat16, jnp.int32, jnp.int16
NN = (((1,), (0,)), ((), ()))
NT = (((1,), (1,)), ((), ()))
TN = (((0,), (0,)), ((), ()))
VMEM = pl.BlockSpec(memory_space=pltpu.VMEM)
SMEM = pl.BlockSpec(memory_space=pltpu.SMEM)
HBM = pl.BlockSpec(memory_space=pltpu.HBM)


def in_hbm(x):
    return pltpu.with_memory_space_constraint(x, pltpu.HBM)


def dot(x, y, dims=NN):
    return lax.dot_general(x, y, dims, preferred_element_type=F32)


def rows_of(shape):
    return lax.broadcasted_iota(I32, shape, 0)


def lanes_of(shape):
    return lax.broadcasted_iota(I32, shape, 1)


def flat(x):
    return jnp.concatenate([x[j : j + 1, :] for j in range(x.shape[0])], axis=1)


def pick(condition, value):
    return jnp.where(condition, value, 0.0).astype(BF16)


def onehot(rows, index, value=None):
    hit = lax.broadcasted_iota(I16, (rows, index.shape[1]), 0) == index.astype(I16)
    one = jnp.ones((), BF16) if value is None else value.astype(BF16)
    return jnp.where(hit, one, jnp.zeros((), BF16))


def counted_before(marks):
    step = jnp.where(
        (rows_of((128, 256)) < lanes_of((128, 256))) | (lanes_of((128, 256)) >= 128), 1.0, 0.0
    ).astype(BF16)
    before, carry = [], jnp.zeros((marks.shape[0], 128), F32)
    for j in range(marks.shape[1] // 128):
        counted = dot(marks[:, 128 * j : 128 * (j + 1)].astype(BF16), step)
        before.append(counted[:, :128] + carry)
        carry = carry + counted[:, 128:]
    return jnp.concatenate(before, axis=1)


def pack_kernel(with_group, me_ref, count_ref, table_ref, key_ref, mult_ref, *rest):
    group_ref = rest[0] if with_group else None
    payload_hbm, out_hbm, payload_ref, out_ref, in_sem, out_sems = rest[-6:]
    rows = DELTA_DEV
    fetch = pltpu.make_async_copy(payload_hbm, payload_ref, in_sem)
    fetch.start()
    key = flat(key_ref[...])
    key_hi, key_lo = key >> 7, key & 127
    low = onehot(128, key_lo)
    table = table_ref[...]
    found = dot((table >> 7).astype(F32).astype(BF16), low) * 128.0 + dot(
        (table & 127).astype(F32).astype(BF16), low
    )
    slot = jnp.sum(jnp.where(rows_of((128, rows)) == key_hi, found, 0.0), axis=0, keepdims=True)
    slot = slot.astype(I32)
    owner, local = slot >> 9, slot & 511
    live = lanes_of((1, rows)) < count_ref[0]
    owner = jnp.where(live, owner, -1)
    marks = jnp.where(rows_of((OWNERS, rows)) == owner, 1.0, 0.0)
    rank = jnp.sum(marks * counted_before(marks), axis=0, keepdims=True).astype(I32)
    position = jnp.where(live, owner * CAP + rank, -1)
    sign = flat(mult_ref[...]).astype(F32)
    field = rows_of((8, rows))
    value = jnp.where(field == 0, local & 255, jnp.where(field == 1, local >> 8, 0))
    if with_group:
        group = flat(group_ref[...])
        value = jnp.where(field == 2, group & 255, jnp.where(field == 3, group >> 8, value))
    value = jnp.broadcast_to(value.astype(F32)[None], (OWNERS, 8, rows)).reshape(8 * OWNERS, rows)
    held = pick((rows_of((8 * OWNERS, rows)) >> 3) == owner, value)
    place = onehot(4 * CAP, rank + CAP * (me_ref[0] % 4))
    fields = dot(held, place, NT).astype(BF16)
    for k in range(OWNERS):
        out_ref[pl.ds(k * BLOCK + CAP, 8), :] = fields[8 * k : 8 * k + 8]
    fetch.wait()
    payload, sent = payload_ref[...], []
    for c in range(OWNERS // 4):
        chosen = onehot(4 * CAP, position - 4 * CAP * c, sign)
        packed = dot(chosen, payload).astype(BF16)
        for j in range(4):
            out_ref[pl.ds((4 * c + j) * BLOCK, CAP), :] = packed[CAP * j : CAP * (j + 1)]
        part = pl.ds(4 * c * BLOCK, 4 * BLOCK)
        sent.append(pltpu.make_async_copy(out_ref.at[part], out_hbm.at[part], out_sems.at[c]))
        sent[-1].start()
    for copy in sent:
        copy.wait()


def pack(me, count, table, key, mult, group, payload):
    extra = [] if group is None else [group.reshape(8, 128)]
    return pl.pallas_call(
        lambda *refs: pack_kernel(group is not None, *refs),
        out_shape=pltpu.HBM((OWNERS * BLOCK, D), BF16),
        in_specs=[SMEM, SMEM] + [VMEM] * (3 + len(extra)) + [HBM],
        out_specs=HBM,
        scratch_shapes=[
            pltpu.VMEM((DELTA_DEV, D), BF16),
            pltpu.VMEM((OWNERS * BLOCK, D), BF16),
            pltpu.SemaphoreType.DMA,
            pltpu.SemaphoreType.DMA((OWNERS // 4,)),
        ],
        compiler_params=LIMIT,
        name="pack_a" if extra else "pack_b",
    )(me, count, *map(in_hbm, (table, key.reshape(8, 128), mult.reshape(8, 128), *extra, payload)))


def fields_of(ref, c):
    total = ref[pl.ds(4 * c * BLOCK + CAP, 8), :].astype(F32)
    for j in range(1, 4):
        total = total + ref[pl.ds((4 * c + j) * BLOCK + CAP, 8), :].astype(F32)
    total = total.astype(I32)
    return total[0:1] + 256 * total[1:2], total[2:3] + 256 * total[3:4]


def payload_of(ref, c):
    return jnp.concatenate(
        [ref[pl.ds((4 * c + j) * BLOCK, CAP), :] for j in range(4)], axis=0
    )


def spread(total_ref, view, outs):
    for s in range(4):
        outs[s][...] = total_ref[pl.ds(((view + s) % 4) * 128, 128), :]


def sum_b_kernel(view_ref, slot_ref, weight_ref, payload_ref, *rest):
    outs, total_ref = rest[:4], rest[4]
    total_ref[...] = jnp.zeros_like(total_ref)
    for c in range(4):
        slot = flat(slot_ref[8 * c : 8 * c + 8, :])
        weight = flat(weight_ref[8 * c : 8 * c + 8, :]).astype(F32)
        chosen = onehot(KEYS_DEV, slot, weight)
        total_ref[...] += dot(chosen, payload_ref[1024 * c : 1024 * (c + 1), :])
    spread(total_ref, view_ref[0], outs)


def sum_db_kernel(view_ref, in_ref, *rest):
    outs, total_ref = rest[:4], rest[4]
    total_ref[...] = jnp.zeros_like(total_ref)
    for c in range(8):
        slot, _ = fields_of(in_ref, c)
        total_ref[...] += dot(onehot(KEYS_DEV, slot), payload_of(in_ref, c))
    spread(total_ref, view_ref[0], outs)


def slices(kernel, view, *args):
    return pl.pallas_call(
        kernel,
        out_shape=[pltpu.HBM((128, D), F32)] + [jax.ShapeDtypeStruct((128, D), F32)] * 3,
        in_specs=[SMEM] + [VMEM] * len(args),
        out_specs=[VMEM] * 4,
        scratch_shapes=[pltpu.VMEM((KEYS_DEV, D), F32)],
        compiler_params=LIMIT,
    )(view, *args)


def shift(x, s):
    return lax.ppermute(x, "view", [(j, (j + s) % 4) for j in range(4)])


def own_total(parts):
    got = [parts[0]] + [shift(parts[s], s) for s in (1, 2, 3)]
    return (got[0] + got[1]) + (got[2] + got[3])


def everyone(x):
    return [x] + [shift(x, s) for s in (1, 2, 3)]


def fill(ref, view, pieces):
    for s in range(4):
        at = pl.ds(((view + 4 - s) % 4) * 128, 128)
        value = pieces(s)
        high = value.astype(BF16)
        ref[at, :D] = high
        ref[at, D:] = (value - high.astype(F32)).astype(BF16)


def terms_of(ref, slot, weight, payload):
    got = dot(onehot(KEYS_DEV, slot, weight), ref[...], TN)
    return (payload.astype(F32) * (got[:, :D] + got[:, D:])).astype(BF16)


def place_of(group, core):
    own = jnp.where(((group >> 7) & 1) == core, GROUPS // 2, 0)
    return own + ((group >> 8) << 7) + (group & 127)


def sort_kernel(h, core_ref, slot_ref, group_ref, weight_ref, payload_hbm, out_ref, field_ref, payload_ref, sem):
    source = payload_hbm.at[pl.ds(h * SORT_RUNS * SORT, SORT_RUNS * SORT)]
    fetch = pltpu.make_async_copy(source, payload_ref, sem)
    fetch.start()
    for s in range(SORT_RUNS):
        first_row = 8 * (h * SORT_RUNS + s)
        rows = slice(first_row, first_row + 8)
        slot, weight = flat(slot_ref[rows, :]), flat(weight_ref[rows, :])
        place = place_of(flat(group_ref[rows, :]), core_ref[0])
        bucket = place >> 6
        shape = (GROUPS // 64, SORT)
        marks = jnp.where(rows_of(shape) == bucket, 1.0, 0.0)
        first = jnp.sum(jnp.where(bucket < rows_of(shape), 1.0, 0.0), axis=1, keepdims=True)
        position = jnp.sum(marks * (counted_before(marks) + first), axis=0, keepdims=True)
        order = onehot(SORT, position.astype(I32))
        if s == 0:
            fetch.wait()
        moved = dot(order, payload_ref[SORT * s : SORT * (s + 1), :]).astype(BF16)
        value, field = jnp.zeros((8, SORT), I32), rows_of((8, SORT))
        for q, part in enumerate((slot & 255, slot >> 8, weight, place & 255, place >> 8)):
            value = jnp.where(field == q, part, value)
        fields = dot(value.astype(F32).astype(BF16), order, NT).astype(I32)
        for j in range(4):
            at = slice(512 * j + 256 * s, 512 * j + 256 * (s + 1))
            part = slice(256 * j, 256 * (j + 1))
            out_ref[at, :] = moved[part]
            field_ref[:, at] = fields[:, part]


def sort(h, core, slot, group, weight, payload):
    rows = SORT_RUNS * SORT
    return pl.pallas_call(
        functools.partial(sort_kernel, h),
        out_shape=[pltpu.HBM((rows, D), BF16), pltpu.HBM((8, rows), I32)],
        in_specs=[SMEM] + [VMEM] * 3 + [HBM],
        out_specs=[VMEM] * 2,
        scratch_shapes=[pltpu.VMEM((rows, D), BF16), pltpu.SemaphoreType.DMA],
        compiler_params=LIMIT,
    )(core, *(in_hbm(x.reshape(32, 128)) for x in (slot, group, weight)), in_hbm(payload))


def join_a_kernel(view_ref, *refs):
    db, sources, outs, table_hbm = refs[:4], refs[4:8], refs[8:10], refs[10]
    table_ref, rows_ref, field_ref, in_sems, out_sems = refs[11:]
    fetched = []
    for h in range(2):
        for n, (source, target) in enumerate(((sources[h + 2], field_ref), (sources[h], rows_ref))):
            fetched.append(pltpu.make_async_copy(source, target.at[h], in_sems.at[2 * h + n]))
            fetched[-1].start()
    sent = []
    for s in range(4):
        at = pl.ds(((view_ref[0] + 4 - s) % 4) * 128, 128)
        sent.append(pltpu.make_async_copy(db[s], table_hbm.at[at], out_sems.at[8 + s]))
        sent[-1].start()
    fill(table_ref, view_ref[0], lambda s: db[s][...])
    for h in range(2):
        fetched[2 * h].wait()
        fetched[2 * h + 1].wait()
        for j in range(4):
            part = pl.ds(512 * j, 512)
            fields = field_ref[h, :, part]
            slot = fields[0:1] + 256 * fields[1:2]
            rows_ref[h, part, :] = terms_of(
                table_ref, slot, fields[2:3].astype(F32), rows_ref[h, part, :]
            )
            sent.append(
                pltpu.make_async_copy(
                    rows_ref.at[h, part], outs[h].at[part], out_sems.at[4 * h + j]
                )
            )
            sent[-1].start()
    for copy in sent:
        copy.wait()


def add_windows(half, total_ref, rows_ref, line_ref, starts, ends):
    base = half * (GROUPS // 2)

    def window(j, at, size):
        chosen = onehot(size, line_ref[j : j + 1, :] - at)
        rows = rows_ref[:, 512 * j : 512 * (j + 1), :].reshape(1024, D)
        total_ref[pl.ds(pl.multiple_of(at - base, 64), size), :] += dot(chosen, rows)

    near = (2 * half, 2 * half + 1)
    first = [jnp.clip(start, base, base + GROUPS // 2) for start in starts]
    for j in near:
        window(j, first[j], WINDOW)
    for j in range(4):
        begin = first[j] + (WINDOW if j in near else 0)
        last = jnp.minimum(ends[j], base + GROUPS // 2 - 1)

        def more(i, carry, j=j, begin=begin):
            window(j, begin + i * STEP, STEP)
            return carry

        lax.fori_loop(0, (last - begin + STEP) // STEP, more, 0)


def join_d_kernel(view_ref, core_ref, *refs):
    db_ref, b, (first, second, fields0, fields1, in_ref) = refs[0], refs[1:5], refs[5:10]
    peer_ref, delta_ref, place_ref, rows_ref, line_ref, bound_ref = refs[10:16]
    whole_ref, field_ref, total_ref, sems = refs[16:]
    copies = [
        pltpu.make_async_copy(source, target, sems.at[n])
        for n, (source, target) in enumerate(
            (
                (fields0, field_ref.at[0]),
                (fields1, field_ref.at[1]),
                (first, rows_ref.at[0]),
                (second, rows_ref.at[1]),
            )
        )
    ]
    for copy in copies:
        copy.start()
    view, core = view_ref[0], core_ref[0]
    fill(
        whole_ref, view, lambda s: b[s][...] + db_ref[pl.ds(((view + 4 - s) % 4) * 128, 128), :]
    )
    for c in range(8):
        slot, group = fields_of(in_ref, c)
        at = slice(256 * c, 256 * (c + 1))
        place_ref[:, at] = place_of(group, core)
        delta_ref[at, :] = terms_of(whole_ref, slot, None, payload_of(in_ref, c))
    copies[0].wait()
    copies[1].wait()
    starts, ends = [], []
    for j in range(4):
        for h in range(2):
            fields = field_ref[h, :, 512 * j : 512 * (j + 1)]
            line_ref[j : j + 1, 512 * h : 512 * (h + 1)] = fields[3:4] + 256 * fields[4:5]
        line = line_ref[j : j + 1, :]
        starts.append((jnp.min(line) >> 6) << 6)
        ends.append(jnp.max(line))
        bound_ref[j], bound_ref[4 + j] = starts[j], ends[j]
    for g in range(GROUPS // 2 // 512):
        chosen = onehot(512, place_ref[...] - 512 * g)
        total_ref[512 * g : 512 * (g + 1), :] = dot(chosen, delta_ref[...])
    total_ref[GROUPS // 2 :, :] = jnp.zeros((WINDOW, D), F32)
    copies[2].wait()
    copies[3].wait()
    add_windows(0, total_ref, rows_ref, line_ref, starts, ends)
    peer_ref[...] = total_ref[: GROUPS // 2, :]


def own_kernel(bound_ref, delta_ref, place_ref, rows_ref, line_ref, out_ref, total_ref):
    for g in range(GROUPS // 2 // 512):
        chosen = onehot(512, place_ref[...] - GROUPS // 2 - 512 * g)
        total_ref[512 * g : 512 * (g + 1), :] = dot(chosen, delta_ref[...])
    total_ref[GROUPS // 2 :, :] = jnp.zeros((WINDOW, D), F32)
    starts, ends = [bound_ref[j] for j in range(4)], [bound_ref[4 + j] for j in range(4)]
    add_windows(1, total_ref, rows_ref, line_ref, starts, ends)
    out_ref[...] = total_ref[: GROUPS // 2, :]


def join(view, core, db, b, halves, received):
    rows = OWNERS * CAP
    table = pltpu.VMEM((KEYS_DEV, 2 * D), BF16)
    total = pltpu.VMEM((GROUPS // 2 + WINDOW, D), F32)
    half = jax.ShapeDtypeStruct((GROUPS // 2, D), F32)
    fields = [in_hbm(halves[h][1]) for h in (0, 1)]
    *terms, db_table = pl.pallas_call(
        join_a_kernel,
        out_shape=[pltpu.HBM((A_DEV // 2, D), BF16)] * 2 + [pltpu.HBM((KEYS_DEV, D), F32)],
        in_specs=[SMEM] + [VMEM] * 4 + [HBM] * 4,
        out_specs=[HBM] * 3,
        scratch_shapes=[
            table,
            pltpu.VMEM((2, A_DEV // 2, D), BF16),
            pltpu.VMEM((2, 8, A_DEV // 2), I32),
            pltpu.SemaphoreType.DMA((4,)),
            pltpu.SemaphoreType.DMA((12,)),
        ],
        compiler_params=LIMIT,
        name="join_a",
    )(view, *db, in_hbm(halves[0][0]), in_hbm(halves[1][0]), *fields)
    peer, delta, place, sorted_rows, line, bound = pl.pallas_call(
        join_d_kernel,
        out_shape=[
            half,
            jax.ShapeDtypeStruct((rows, D), BF16),
            jax.ShapeDtypeStruct((1, rows), I32),
            jax.ShapeDtypeStruct((2, A_DEV // 2, D), BF16),
            jax.ShapeDtypeStruct((4, 1024), I32),
            jax.ShapeDtypeStruct((8,), I32),
        ],
        in_specs=[SMEM] * 2 + [VMEM] * 5 + [HBM] * 4 + [VMEM],
        out_specs=[VMEM] * 5 + [SMEM],
        scratch_shapes=[
            table,
            pltpu.VMEM((2, 8, A_DEV // 2), I32),
            total,
            pltpu.SemaphoreType.DMA((4,)),
        ],
        compiler_params=pltpu.CompilerParams(vmem_limit_bytes=28 * 2**20),
        name="join_d",
    )(view, core, in_hbm(db_table), *b, *map(in_hbm, terms), *fields, received)
    other = lax.ppermute(peer, "keys_2", [(0, 1), (1, 0)])
    own = pl.pallas_call(
        own_kernel,
        out_shape=half,
        in_specs=[SMEM] + [VMEM] * 4,
        out_specs=VMEM,
        scratch_shapes=[total],
        compiler_params=LIMIT,
        name="join_own",
    )(bound, delta, place, sorted_rows, line)
    return (own + other).astype(BF16)


def exchange(packed):
    blocks = packed.reshape(OWNERS, BLOCK, D)
    return lax.all_to_all(blocks, KEYS, 0, 0, tiled=True).reshape(OWNERS * BLOCK, D)


def shards(
    key_slot,
    a_slot,
    a_group,
    a_weight,
    a_payload,
    b_slot,
    b_weight,
    b_payload,
    da_key,
    da_group,
    da_mult,
    da_payload,
    da_count,
    db_key,
    db_mult,
    db_payload,
    db_count,
):
    me = lax.axis_index(KEYS).astype(I32).reshape(1)
    view = lax.axis_index("view").astype(I32).reshape(1)
    table = key_slot.reshape(128, 128)
    core = lax.axis_index("keys_2").astype(I32).reshape(1)
    db_out = pack(me, db_count, table, db_key, db_mult, None, db_payload)
    da_out = pack(me, da_count, table, da_key, da_mult, da_group, da_payload)
    db_in = exchange(db_out)
    da_in = exchange(da_out)
    b_parts = slices(
        sum_b_kernel, view, b_slot.reshape(32, 128), b_weight.reshape(32, 128), b_payload
    )
    b = everyone(own_total(b_parts))
    db = everyone(own_total(slices(sum_db_kernel, view, db_in)))
    halves = [sort(h, core, a_slot, a_group, a_weight, a_payload) for h in (0, 1)]
    partial = join(view, core, db, b, halves, da_in)
    blocks = partial.reshape(GROUPS // 2 // GROUPS_DEV, GROUPS_DEV, D)
    blocks = lax.all_to_all(blocks, ("keys_0", "keys_1", "view"), 0, 0, tiled=True)
    return jnp.sum(blocks.astype(F32), axis=0)


def solution(mesh):
    split = Mesh(
        mesh.devices.reshape(4, 4, 2, mesh.shape["view"]), ("keys_0", "keys_1", "keys_2", "view")
    )
    one, two = P(KEYS_VIEW), P(KEYS_VIEW, None)
    placed = (
        P(), one, one, one, two, one, one, two, one, one, one, two, one, one, one, two, one,
    )
    return jax.shard_map(shards, mesh=split, in_specs=placed, out_specs=two, check_vma=False)
```

```python
import jax
import jax.numpy as jnp
from jax import lax
from jax.experimental import pallas as pl
from jax.experimental.pallas import tpu as pltpu
from jax.sharding import Mesh
from jax.sharding import PartitionSpec as P


KEYS_DEV = 512
GROUPS_DEV = 32
GROUPS = 4096
DELTA_DEV = 1024
A_DEV = 4096
D = 256
OWNERS = 32
CAP = 64
BLOCK = CAP + 8
SORT, RUNS = 512, 8
WINDOW = 1472
STEP = 256
LIMIT = pltpu.CompilerParams(vmem_limit_bytes=16 * 2**20)
KEYS = ("keys_0", "keys_1", "keys_2")
KEYS_VIEW = ("keys_0", "keys_1", "keys_2", "view")
F32, BF16, I32, I16 = jnp.float32, jnp.bfloat16, jnp.int32, jnp.int16
NN = (((1,), (0,)), ((), ()))
NT = (((1,), (1,)), ((), ()))
TN = (((0,), (0,)), ((), ()))
VMEM = pl.BlockSpec(memory_space=pltpu.VMEM)
SMEM = pl.BlockSpec(memory_space=pltpu.SMEM)
HBM = pl.BlockSpec(memory_space=pltpu.HBM)


def in_hbm(x):
    return pltpu.with_memory_space_constraint(x, pltpu.HBM)


def dot(x, y, dims=NN):
    return lax.dot_general(x, y, dims, preferred_element_type=F32)


def rows_of(shape):
    return lax.broadcasted_iota(I32, shape, 0)


def lanes_of(shape):
    return lax.broadcasted_iota(I32, shape, 1)


def flat(x):
    return jnp.concatenate([x[j : j + 1, :] for j in range(x.shape[0])], axis=1)


def pick(condition, value):
    return jnp.where(condition, value, 0.0).astype(BF16)


def onehot(rows, index, value=None):
    hit = lax.broadcasted_iota(I16, (rows, index.shape[1]), 0) == index.astype(I16)
    one = jnp.ones((), BF16) if value is None else value.astype(BF16)
    return jnp.where(hit, one, jnp.zeros((), BF16))


def counted_before(marks):
    step = jnp.where(
        (rows_of((128, 256)) < lanes_of((128, 256))) | (lanes_of((128, 256)) >= 128), 1.0, 0.0
    ).astype(BF16)
    before, carry = [], jnp.zeros((marks.shape[0], 128), F32)
    for j in range(marks.shape[1] // 128):
        counted = dot(marks[:, 128 * j : 128 * (j + 1)].astype(BF16), step)
        before.append(counted[:, :128] + carry)
        carry = carry + counted[:, 128:]
    return jnp.concatenate(before, axis=1)


def pack_kernel(with_group, me_ref, count_ref, table_ref, key_ref, mult_ref, *rest):
    group_ref = rest[0] if with_group else None
    payload_hbm, out_ref, payload_ref, in_sem = rest[-4:]
    rows = DELTA_DEV
    fetch = pltpu.make_async_copy(payload_hbm, payload_ref, in_sem)
    fetch.start()
    key = flat(key_ref[...])
    key_hi, key_lo = key >> 7, key & 127
    low = onehot(128, key_lo)
    table = table_ref[...]
    found = dot((table >> 7).astype(F32).astype(BF16), low) * 128.0 + dot(
        (table & 127).astype(F32).astype(BF16), low
    )
    slot = jnp.sum(jnp.where(rows_of((128, rows)) == key_hi, found, 0.0), axis=0, keepdims=True)
    slot = slot.astype(I32)
    owner, local = slot >> 9, slot & 511
    live = lanes_of((1, rows)) < count_ref[0]
    owner = jnp.where(live, owner, -1)
    marks = jnp.where(rows_of((OWNERS, rows)) == owner, 1.0, 0.0)
    rank = jnp.sum(marks * counted_before(marks), axis=0, keepdims=True).astype(I32)
    position = jnp.where(live, owner * CAP + rank, -1)
    sign = flat(mult_ref[...]).astype(F32)
    field = rows_of((8, rows))
    value = jnp.where(field == 0, local & 255, jnp.where(field == 1, local >> 8, 0))
    if with_group:
        group = flat(group_ref[...])
        value = jnp.where(field == 2, group & 255, jnp.where(field == 3, group >> 8, value))
    value = jnp.broadcast_to(value.astype(F32)[None], (OWNERS, 8, rows)).reshape(8 * OWNERS, rows)
    held = pick((rows_of((8 * OWNERS, rows)) >> 3) == owner, value)
    place = onehot(4 * CAP, rank + CAP * (me_ref[0] % 4))
    fields = dot(held, place, NT).astype(BF16)
    for k in range(OWNERS):
        out_ref[pl.ds(k * BLOCK + CAP, 8), :] = fields[8 * k : 8 * k + 8]
    fetch.wait()
    payload = payload_ref[...]
    for c in range(OWNERS // 4):
        chosen = onehot(4 * CAP, position - 4 * CAP * c, sign)
        packed = dot(chosen, payload).astype(BF16)
        for j in range(4):
            out_ref[pl.ds((4 * c + j) * BLOCK, CAP), :] = packed[CAP * j : CAP * (j + 1)]


def pack(me, count, table, key, mult, group, payload):
    extra = [] if group is None else [group.reshape(8, 128)]
    return pl.pallas_call(
        lambda *refs: pack_kernel(group is not None, *refs),
        out_shape=jax.ShapeDtypeStruct((OWNERS * BLOCK, D), BF16),
        in_specs=[SMEM, SMEM] + [VMEM] * (3 + len(extra)) + [HBM],
        out_specs=VMEM,
        scratch_shapes=[pltpu.VMEM((DELTA_DEV, D), BF16), pltpu.SemaphoreType.DMA],
        compiler_params=LIMIT,
        name="pack_a" if extra else "pack_b",
    )(me, count, *map(in_hbm, (table, key.reshape(8, 128), mult.reshape(8, 128), *extra, payload)))


def fields_of(ref, c):
    total = ref[pl.ds(4 * c * BLOCK + CAP, 8), :].astype(F32)
    for j in range(1, 4):
        total = total + ref[pl.ds((4 * c + j) * BLOCK + CAP, 8), :].astype(F32)
    total = total.astype(I32)
    return total[0:1] + 256 * total[1:2], total[2:3] + 256 * total[3:4]


def payload_of(ref, c):
    return jnp.concatenate(
        [ref[pl.ds((4 * c + j) * BLOCK, CAP), :] for j in range(4)], axis=0
    )


def spread(total_ref, view, outs):
    for s in range(4):
        outs[s][...] = total_ref[pl.ds(((view + s) % 4) * 128, 128), :]


def sum_b_kernel(view_ref, slot_ref, weight_ref, payload_ref, *rest):
    outs, total_ref = rest[:4], rest[4]
    total_ref[...] = jnp.zeros_like(total_ref)
    for c in range(4):
        slot = flat(slot_ref[8 * c : 8 * c + 8, :])
        weight = flat(weight_ref[8 * c : 8 * c + 8, :]).astype(F32)
        chosen = onehot(KEYS_DEV, slot, weight)
        total_ref[...] += dot(chosen, payload_ref[1024 * c : 1024 * (c + 1), :])
    spread(total_ref, view_ref[0], outs)


def sum_db_kernel(view_ref, in_ref, *rest):
    outs, total_ref = rest[:4], rest[4]
    total_ref[...] = jnp.zeros_like(total_ref)
    for c in range(8):
        slot, _ = fields_of(in_ref, c)
        total_ref[...] += dot(onehot(KEYS_DEV, slot), payload_of(in_ref, c))
    spread(total_ref, view_ref[0], outs)


def slices(kernel, view, *args):
    return pl.pallas_call(
        kernel,
        out_shape=[pltpu.HBM((128, D), F32)] + [jax.ShapeDtypeStruct((128, D), F32)] * 3,
        in_specs=[SMEM] + [VMEM] * len(args),
        out_specs=[VMEM] * 4,
        scratch_shapes=[pltpu.VMEM((KEYS_DEV, D), F32)],
        compiler_params=LIMIT,
    )(view, *args)


def shift(x, s):
    return lax.ppermute(x, "view", [(j, (j + s) % 4) for j in range(4)])


def own_total(parts):
    got = [parts[0]] + [shift(parts[s], s) for s in (1, 2, 3)]
    return (got[0] + got[1]) + (got[2] + got[3])


def everyone(x):
    return [x] + [shift(x, s) for s in (1, 2, 3)]


def fill(ref, view, pieces):
    for s in range(4):
        at = pl.ds(((view + 4 - s) % 4) * 128, 128)
        value = pieces(s)
        high = value.astype(BF16)
        ref[at, :D] = high
        ref[at, D:] = (value - high.astype(F32)).astype(BF16)


def terms_of(ref, slot, weight, payload):
    got = dot(onehot(KEYS_DEV, slot, weight), ref[...], TN)
    return (payload.astype(F32) * (got[:, :D] + got[:, D:])).astype(BF16)


def place_of(group, core):
    own = jnp.where(((group >> 7) & 1) == core, GROUPS // 2, 0)
    return own + ((group >> 8) << 7) + (group & 127)


def sort_kernel(
    core_ref, slot_ref, group_ref, weight_ref, payload_hbm, out_ref, field_ref, payload_ref, sems
):
    fetched = []
    for s in range(RUNS):
        part = pl.ds(SORT * s, SORT)
        fetched.append(
            pltpu.make_async_copy(payload_hbm.at[part], payload_ref.at[part], sems.at[s])
        )
        fetched[-1].start()
    buckets, quarter = GROUPS // 64, SORT // 4
    places = place_of(group_ref[...], core_ref[0])

    def run_of(x, s):
        return flat(x[SORT // 128 * s : SORT // 128 * (s + 1), :])

    bucket = [run_of(places, s) >> 6 for s in range(RUNS)]
    number = rows_of((buckets, SORT))
    marks = [jnp.where(number == k, 1.0, 0.0) for k in bucket]
    first = [jnp.sum(jnp.where(k < number, 1.0, 0.0), axis=1, keepdims=True) for k in bucket]
    before = counted_before(jnp.concatenate(marks, axis=0)) + jnp.concatenate(first, axis=0)
    position = [
        jnp.sum(marks[s] * before[buckets * s : buckets * (s + 1)], axis=0, keepdims=True)
        for s in range(RUNS)
    ]
    position = [p.astype(I32) for p in position]
    row, found = rows_of((24, SORT)), []
    for s in range(RUNS):
        slot, weight, place = (run_of(x, s) for x in (slot_ref[...], weight_ref[...], places))
        value = jnp.zeros((24, SORT), I32)
        for q, part in enumerate((slot & 255, slot >> 8, weight, place & 255, place >> 8)):
            value = jnp.where((row >> 2) == q, part, value)
        held = pick((row & 3) == position[s] // quarter, value.astype(F32))
        found.append(dot(held, onehot(quarter, position[s] % quarter), NT).astype(I32))
    for s in range(RUNS):
        at, f = slice(quarter * s, quarter * (s + 1)), found[s]
        field_ref[0:4, at] = f[0:4] + 256 * f[4:8]
        field_ref[4:8, at] = f[8:12]
        field_ref[8:12, at] = f[12:16] + 256 * f[16:20]
        field_ref[12:16, at] = jnp.zeros((4, quarter), I32)
    for s in range(RUNS):
        fetched[s].wait()
        moved = dot(onehot(SORT, position[s]), payload_ref[SORT * s : SORT * (s + 1), :])
        for j in range(4):
            out_ref[j, quarter * s : quarter * (s + 1), :] = moved[
                quarter * j : quarter * (j + 1)
            ].astype(BF16)


def sort(core, slot, group, weight, payload):
    return pl.pallas_call(
        sort_kernel,
        out_shape=[
            jax.ShapeDtypeStruct((4, A_DEV // 4, D), BF16),
            jax.ShapeDtypeStruct((16, A_DEV // 4), I32),
        ],
        in_specs=[SMEM] + [VMEM] * 3 + [HBM],
        out_specs=[VMEM] * 2,
        scratch_shapes=[pltpu.VMEM((A_DEV, D), BF16), pltpu.SemaphoreType.DMA((RUNS,))],
        compiler_params=LIMIT,
        name="sort",
    )(core, *(in_hbm(x.reshape(32, 128)) for x in (slot, group, weight)), in_hbm(payload))


def join_a_kernel(view_ref, *refs):
    db, (sorted_ref, field_ref), (terms_hbm, field_hbm, table_hbm) = refs[:4], refs[4:6], refs[6:9]
    table_ref, rows_ref, sems = refs[9:]
    sent = [pltpu.make_async_copy(field_ref, field_hbm, sems.at[8])]
    for s in range(4):
        at = pl.ds(((view_ref[0] + 4 - s) % 4) * 128, 128)
        sent.append(pltpu.make_async_copy(db[s], table_hbm.at[at], sems.at[4 + s]))
    for copy in sent:
        copy.start()
    fill(table_ref, view_ref[0], lambda s: db[s][...])
    for j in range(4):
        weight = field_ref[4 + j : 5 + j, :].astype(F32)
        rows_ref[j] = terms_of(table_ref, field_ref[j : j + 1, :], weight, sorted_ref[j])
        sent.append(pltpu.make_async_copy(rows_ref.at[j], terms_hbm.at[j], sems.at[j]))
        sent[-1].start()
    for copy in sent:
        copy.wait()


def add_windows(half, total_ref, rows_ref, line_ref, starts, ends):
    base = half * (GROUPS // 2)

    def window(j, at, size):
        chosen = onehot(size, line_ref[j : j + 1, :] - at)
        total_ref[pl.ds(pl.multiple_of(at - base, 64), size), :] += dot(chosen, rows_ref[j])

    near = (2 * half, 2 * half + 1)
    first = [jnp.clip(start, base, base + GROUPS // 2) for start in starts]
    for j in near:
        window(j, first[j], WINDOW)
    for j in range(4):
        begin = first[j] + (WINDOW if j in near else 0)
        last = jnp.minimum(ends[j], base + GROUPS // 2 - 1)

        def more(i, carry, j=j, begin=begin):
            window(j, begin + i * STEP, STEP)
            return carry

        lax.fori_loop(0, (last - begin + STEP) // STEP, more, 0)


def add_deltas(half, total_ref, place_ref, delta_ref):
    for g in range(2):
        chosen = onehot(1024, place_ref[...] - (half * (GROUPS // 2) + 1024 * g))
        total_ref[1024 * g : 1024 * (g + 1), :] = dot(chosen, delta_ref[...])
    total_ref[GROUPS // 2 :, :] = jnp.zeros((WINDOW, D), F32)


def join_d_kernel(view_ref, core_ref, *refs):
    db_hbm, b, (field_hbm, terms_hbm, in_ref) = refs[0], refs[1:5], refs[5:8]
    peer_ref, delta_ref, place_ref, rows_ref, line_ref, bound_ref = refs[8:14]
    whole_ref, total_ref, db_ref, b_ref, field_ref, sems = refs[14:]
    view, core = view_ref[0], core_ref[0]
    tables = [pltpu.make_async_copy(db_hbm, db_ref, sems.at[0])]
    for s in range(4):
        at = pl.ds(((view + 4 - s) % 4) * 128, 128)
        tables.append(pltpu.make_async_copy(b[s], b_ref.at[at], sems.at[1 + s]))
    fields = pltpu.make_async_copy(field_hbm, field_ref, sems.at[5])
    terms = pltpu.make_async_copy(terms_hbm, rows_ref, sems.at[6])
    for copy in (*tables, fields, terms):
        copy.start()
    slots = []
    for c in range(8):
        slot, group = fields_of(in_ref, c)
        place_ref[:, 256 * c : 256 * (c + 1)] = place_of(group, core)
        slots.append(slot)
    for copy in tables:
        copy.wait()
    whole = b_ref[...] + db_ref[...]
    high = whole.astype(BF16)
    whole_ref[:, :D] = high
    whole_ref[:, D:] = (whole - high.astype(F32)).astype(BF16)
    for c in range(8):
        at = slice(256 * c, 256 * (c + 1))
        delta_ref[at, :] = terms_of(whole_ref, slots[c], None, payload_of(in_ref, c))
    fields.wait()
    starts, ends = [], []
    for j in range(4):
        line = field_ref[8 + j : 9 + j, :]
        line_ref[j : j + 1, :] = line
        starts.append((jnp.min(line) >> 6) << 6)
        ends.append(jnp.max(line))
        bound_ref[j], bound_ref[4 + j] = starts[j], ends[j]
    add_deltas(0, total_ref, place_ref, delta_ref)
    terms.wait()
    add_windows(0, total_ref, rows_ref, line_ref, starts, ends)
    peer_ref[...] = total_ref[: GROUPS // 2, :]


def own_kernel(bound_ref, delta_ref, place_ref, rows_ref, line_ref, out_ref, total_ref):
    add_deltas(1, total_ref, place_ref, delta_ref)
    starts, ends = [bound_ref[j] for j in range(4)], [bound_ref[4 + j] for j in range(4)]
    add_windows(1, total_ref, rows_ref, line_ref, starts, ends)
    out_ref[...] = total_ref[: GROUPS // 2, :]


def join(view, core, db, b, sorted_rows, received):
    rows = OWNERS * CAP
    table = pltpu.VMEM((KEYS_DEV, 2 * D), BF16)
    total = pltpu.VMEM((GROUPS // 2 + WINDOW, D), F32)
    half = jax.ShapeDtypeStruct((GROUPS // 2, D), F32)
    terms, fields, db_table = pl.pallas_call(
        join_a_kernel,
        out_shape=[
            pltpu.HBM((4, A_DEV // 4, D), BF16),
            pltpu.HBM((16, A_DEV // 4), I32),
            pltpu.HBM((KEYS_DEV, D), F32),
        ],
        in_specs=[SMEM] + [VMEM] * 6,
        out_specs=[HBM] * 3,
        scratch_shapes=[
            table,
            pltpu.VMEM((4, A_DEV // 4, D), BF16),
            pltpu.SemaphoreType.DMA((9,)),
        ],
        compiler_params=LIMIT,
        name="join_a",
    )(view, *db, *sorted_rows)
    peer, delta, place, term_rows, line, bound = pl.pallas_call(
        join_d_kernel,
        out_shape=[
            half,
            jax.ShapeDtypeStruct((rows, D), BF16),
            jax.ShapeDtypeStruct((1, rows), I32),
            jax.ShapeDtypeStruct((4, A_DEV // 4, D), BF16),
            jax.ShapeDtypeStruct((4, A_DEV // 4), I32),
            jax.ShapeDtypeStruct((8,), I32),
        ],
        in_specs=[SMEM] * 2 + [HBM] * 7 + [VMEM],
        out_specs=[VMEM] * 5 + [SMEM],
        scratch_shapes=[
            table,
            total,
            pltpu.VMEM((KEYS_DEV, D), F32),
            pltpu.VMEM((KEYS_DEV, D), F32),
            pltpu.VMEM((16, A_DEV // 4), I32),
            pltpu.SemaphoreType.DMA((7,)),
        ],
        compiler_params=pltpu.CompilerParams(vmem_limit_bytes=28 * 2**20),
        name="join_d",
    )(view, core, *map(in_hbm, (db_table, *b, fields, terms)), received)
    other = lax.ppermute(peer, "keys_2", [(0, 1), (1, 0)])
    own = pl.pallas_call(
        own_kernel,
        out_shape=half,
        in_specs=[SMEM] + [VMEM] * 4,
        out_specs=VMEM,
        scratch_shapes=[total],
        compiler_params=LIMIT,
        name="join_own",
    )(bound, delta, place, term_rows, line)
    return (own + other).astype(BF16)


def exchange(packed):
    blocks = packed.reshape(OWNERS, BLOCK, D)
    return lax.all_to_all(blocks, KEYS, 0, 0, tiled=True).reshape(OWNERS * BLOCK, D)


def shards(
    key_slot,
    a_slot,
    a_group,
    a_weight,
    a_payload,
    b_slot,
    b_weight,
    b_payload,
    da_key,
    da_group,
    da_mult,
    da_payload,
    da_count,
    db_key,
    db_mult,
    db_payload,
    db_count,
):
    me = lax.axis_index(KEYS).astype(I32).reshape(1)
    view = lax.axis_index("view").astype(I32).reshape(1)
    table = key_slot.reshape(128, 128)
    core = lax.axis_index("keys_2").astype(I32).reshape(1)
    db_out = pack(me, db_count, table, db_key, db_mult, None, db_payload)
    da_out = pack(me, da_count, table, da_key, da_mult, da_group, da_payload)
    db_in = exchange(db_out)
    da_in = exchange(da_out)
    b_parts = slices(
        sum_b_kernel, view, b_slot.reshape(32, 128), b_weight.reshape(32, 128), b_payload
    )
    b = everyone(own_total(b_parts))
    db = everyone(own_total(slices(sum_db_kernel, view, db_in)))
    sorted_rows = sort(core, a_slot, a_group, a_weight, a_payload)
    partial = join(view, core, db, b, sorted_rows, da_in)
    blocks = partial.reshape(GROUPS // 2 // GROUPS_DEV, GROUPS_DEV, D)
    blocks = lax.all_to_all(blocks, ("keys_0", "keys_1", "view"), 0, 0, tiled=True)
    return jnp.sum(blocks.astype(F32), axis=0)


def solution(mesh):
    split = Mesh(
        mesh.devices.reshape(4, 4, 2, mesh.shape["view"]), ("keys_0", "keys_1", "keys_2", "view")
    )
    one, two = P(KEYS_VIEW), P(KEYS_VIEW, None)
    placed = (
        P(), one, one, one, two, one, one, two, one, one, one, two, one, one, one, two, one,
    )
    return jax.shard_map(shards, mesh=split, in_specs=placed, out_specs=two, check_vma=False)
```

```python
import jax
import jax.numpy as jnp
from jax import lax
from jax.experimental import pallas as pl
from jax.experimental.pallas import tpu as pltpu
from jax.sharding import Mesh
from jax.sharding import PartitionSpec as P


KEYS_DEV = 512
GROUPS_DEV = 32
GROUPS = 4096
DELTA_DEV = 1024
A_DEV = 4096
D = 256
OWNERS = 32
CAP = 64
BLOCK = CAP + 8
SORT, RUNS = 512, 8
PARTS = 8
WINDOW = 1024
STEP = 256
LIMIT = pltpu.CompilerParams(vmem_limit_bytes=16 * 2**20)
KEYS = ("keys_0", "keys_1", "keys_2")
KEYS_VIEW = ("keys_0", "keys_1", "keys_2", "view")
F32, BF16, I32, I16 = jnp.float32, jnp.bfloat16, jnp.int32, jnp.int16
NN = (((1,), (0,)), ((), ()))
NT = (((1,), (1,)), ((), ()))
TN = (((0,), (0,)), ((), ()))
VMEM = pl.BlockSpec(memory_space=pltpu.VMEM)
SMEM = pl.BlockSpec(memory_space=pltpu.SMEM)
HBM = pl.BlockSpec(memory_space=pltpu.HBM)


def in_hbm(x):
    return pltpu.with_memory_space_constraint(x, pltpu.HBM)


def dot(x, y, dims=NN):
    return lax.dot_general(x, y, dims, preferred_element_type=F32)


def rows_of(shape):
    return lax.broadcasted_iota(I32, shape, 0)


def lanes_of(shape):
    return lax.broadcasted_iota(I32, shape, 1)


def flat(x):
    return jnp.concatenate([x[j : j + 1, :] for j in range(x.shape[0])], axis=1)


def pick(condition, value):
    return jnp.where(condition, value, 0.0).astype(BF16)


def onehot(rows, index, value=None):
    hit = lax.broadcasted_iota(I16, (rows, index.shape[1]), 0) == index.astype(I16)
    one = jnp.ones((), BF16) if value is None else value.astype(BF16)
    return jnp.where(hit, one, jnp.zeros((), BF16))


def counted_before(marks):
    step = jnp.where(
        (rows_of((128, 256)) < lanes_of((128, 256))) | (lanes_of((128, 256)) >= 128), 1.0, 0.0
    ).astype(BF16)
    before, carry = [], jnp.zeros((marks.shape[0], 128), F32)
    for j in range(marks.shape[1] // 128):
        counted = dot(marks[:, 128 * j : 128 * (j + 1)].astype(BF16), step)
        before.append(counted[:, :128] + carry)
        carry = carry + counted[:, 128:]
    return jnp.concatenate(before, axis=1)


def pack_kernel(with_group, me_ref, count_ref, table_ref, key_ref, mult_ref, *rest):
    group_ref = rest[0] if with_group else None
    payload_hbm, out_hbm, payload_ref, out_ref, in_sem, out_sems = rest[-6:]
    rows = DELTA_DEV
    fetch = pltpu.make_async_copy(payload_hbm, payload_ref, in_sem)
    fetch.start()
    key = flat(key_ref[...])
    key_hi, key_lo = key >> 7, key & 127
    low = onehot(128, key_lo)
    table = table_ref[...]
    found = dot((table >> 7).astype(F32).astype(BF16), low) * 128.0 + dot(
        (table & 127).astype(F32).astype(BF16), low
    )
    slot = jnp.sum(jnp.where(rows_of((128, rows)) == key_hi, found, 0.0), axis=0, keepdims=True)
    slot = slot.astype(I32)
    owner, local = slot >> 9, slot & 511
    live = lanes_of((1, rows)) < count_ref[0]
    owner = jnp.where(live, owner, -1)
    marks = jnp.where(rows_of((OWNERS, rows)) == owner, 1.0, 0.0)
    rank = jnp.sum(marks * counted_before(marks), axis=0, keepdims=True).astype(I32)
    position = jnp.where(live, owner * CAP + rank, -1)
    sign = flat(mult_ref[...]).astype(F32)
    field = rows_of((8, rows))
    value = jnp.where(field == 0, local & 255, jnp.where(field == 1, local >> 8, 0))
    if with_group:
        group = flat(group_ref[...])
        value = jnp.where(field == 2, group & 255, jnp.where(field == 3, group >> 8, value))
    value = jnp.broadcast_to(value.astype(F32)[None], (OWNERS, 8, rows)).reshape(8 * OWNERS, rows)
    held = pick((rows_of((8 * OWNERS, rows)) >> 3) == owner, value)
    place = onehot(4 * CAP, rank + CAP * (me_ref[0] % 4))
    fields = dot(held, place, NT).astype(BF16)
    for k in range(OWNERS):
        out_ref[pl.ds(k * BLOCK + CAP, 8), :] = fields[8 * k : 8 * k + 8]
    fetch.wait()
    payload, sent = payload_ref[...], []
    for c in range(OWNERS // 4):
        chosen = onehot(4 * CAP, position - 4 * CAP * c, sign)
        packed = dot(chosen, payload).astype(BF16)
        for j in range(4):
            out_ref[pl.ds((4 * c + j) * BLOCK, CAP), :] = packed[CAP * j : CAP * (j + 1)]
        part = pl.ds(4 * c * BLOCK, 4 * BLOCK)
        sent.append(pltpu.make_async_copy(out_ref.at[part], out_hbm.at[part], out_sems.at[c]))
        sent[-1].start()
    for copy in sent:
        copy.wait()


def pack(me, count, table, key, mult, group, payload):
    extra = [] if group is None else [group.reshape(8, 128)]
    return pl.pallas_call(
        lambda *refs: pack_kernel(group is not None, *refs),
        out_shape=pltpu.HBM((OWNERS * BLOCK, D), BF16),
        in_specs=[SMEM, SMEM] + [VMEM] * (3 + len(extra)) + [HBM],
        out_specs=HBM,
        scratch_shapes=[
            pltpu.VMEM((DELTA_DEV, D), BF16),
            pltpu.VMEM((OWNERS * BLOCK, D), BF16),
            pltpu.SemaphoreType.DMA,
            pltpu.SemaphoreType.DMA((OWNERS // 4,)),
        ],
        compiler_params=LIMIT,
        name="pack_a" if extra else "pack_b",
    )(me, count, *map(in_hbm, (table, key.reshape(8, 128), mult.reshape(8, 128), *extra, payload)))


def fields_of(ref, c):
    total = ref[pl.ds(4 * c * BLOCK + CAP, 8), :].astype(F32)
    for j in range(1, 4):
        total = total + ref[pl.ds((4 * c + j) * BLOCK + CAP, 8), :].astype(F32)
    total = total.astype(I32)
    return total[0:1] + 256 * total[1:2], total[2:3] + 256 * total[3:4]


def payload_of(ref, c):
    return jnp.concatenate(
        [ref[pl.ds((4 * c + j) * BLOCK, CAP), :] for j in range(4)], axis=0
    )


def spread(total_ref, view, outs):
    for s in range(4):
        outs[s][...] = total_ref[pl.ds(((view + s) % 4) * 128, 128), :]


def sum_b_kernel(view_ref, slot_ref, weight_ref, payload_ref, *rest):
    outs, total_ref = rest[:4], rest[4]
    total_ref[...] = jnp.zeros_like(total_ref)
    for c in range(4):
        slot = flat(slot_ref[8 * c : 8 * c + 8, :])
        weight = flat(weight_ref[8 * c : 8 * c + 8, :]).astype(F32)
        chosen = onehot(KEYS_DEV, slot, weight)
        total_ref[...] += dot(chosen, payload_ref[1024 * c : 1024 * (c + 1), :])
    spread(total_ref, view_ref[0], outs)


def sum_db_kernel(view_ref, in_ref, *rest):
    outs, total_ref = rest[:4], rest[4]
    total_ref[...] = jnp.zeros_like(total_ref)
    for c in range(8):
        slot, _ = fields_of(in_ref, c)
        total_ref[...] += dot(onehot(KEYS_DEV, slot), payload_of(in_ref, c))
    spread(total_ref, view_ref[0], outs)


def slices(kernel, view, own, *args):
    return pl.pallas_call(
        kernel,
        out_shape=[own((128, D), F32)] + [jax.ShapeDtypeStruct((128, D), F32)] * 3,
        in_specs=[SMEM] + [VMEM] * len(args),
        out_specs=[VMEM] * 4,
        scratch_shapes=[pltpu.VMEM((KEYS_DEV, D), F32)],
        compiler_params=LIMIT,
    )(view, *args)


def shift(x, s):
    return lax.ppermute(x, "view", [(j, (j + s) % 4) for j in range(4)])


def own_total(parts):
    got = [parts[0]] + [shift(parts[s], s) for s in (1, 2, 3)]
    return (got[0] + got[1]) + (got[2] + got[3])


def everyone(x):
    return [x] + [shift(x, s) for s in (1, 2, 3)]


def fill(ref, view, pieces):
    for s in range(4):
        at = pl.ds(((view + 4 - s) % 4) * 128, 128)
        value = pieces(s)
        high = value.astype(BF16)
        ref[at, :D] = high
        ref[at, D:] = (value - high.astype(F32)).astype(BF16)


def terms_of(ref, slot, weight, payload):
    got = dot(onehot(KEYS_DEV, slot, weight), ref[...], TN)
    return (payload.astype(F32) * (got[:, :D] + got[:, D:])).astype(BF16)


def place_of(group, core):
    own = jnp.where(((group >> 7) & 1) == core, GROUPS // 2, 0)
    return own + ((group >> 8) << 7) + (group & 127)


def sort_kernel(
    core_ref, slot_ref, group_ref, weight_ref, payload_hbm, out_ref, field_ref, payload_ref, sems
):
    fetched = []
    for s in range(RUNS):
        part = pl.ds(SORT * s, SORT)
        fetched.append(
            pltpu.make_async_copy(payload_hbm.at[part], payload_ref.at[part], sems.at[s])
        )
        fetched[-1].start()
    buckets, part_rows = GROUPS // 64, SORT // PARTS
    places = place_of(group_ref[...], core_ref[0])

    def run_of(x, s):
        return flat(x[SORT // 128 * s : SORT // 128 * (s + 1), :])

    bucket = [run_of(places, s) >> 6 for s in range(RUNS)]
    number = rows_of((buckets, SORT))
    marks = [jnp.where(number == k, 1.0, 0.0) for k in bucket]
    first = [jnp.sum(jnp.where(k < number, 1.0, 0.0), axis=1, keepdims=True) for k in bucket]
    before = counted_before(jnp.concatenate(marks, axis=0)) + jnp.concatenate(first, axis=0)
    position = [
        jnp.sum(marks[s] * before[buckets * s : buckets * (s + 1)], axis=0, keepdims=True)
        for s in range(RUNS)
    ]
    position = [p.astype(I32) for p in position]
    row, found = rows_of((5 * PARTS, SORT)), []
    for s in range(RUNS):
        slot, weight, place = (run_of(x, s) for x in (slot_ref[...], weight_ref[...], places))
        value = jnp.zeros((5 * PARTS, SORT), I32)
        for q, part in enumerate((slot & 255, slot >> 8, weight, place & 255, place >> 8)):
            value = jnp.where((row >> 3) == q, part, value)
        held = pick((row & 7) == position[s] >> 6, value.astype(F32))
        lane = (position[s] & 63) + part_rows * (s % 2)
        found.append(dot(held, onehot(2 * part_rows, lane), NT))
    for s in range(0, RUNS, 2):
        at = slice(part_rows * s, part_rows * (s + 2))
        f = (found[s] + found[s + 1]).astype(I32)
        field_ref[0:8, at] = f[0:8] + 256 * f[8:16]
        field_ref[8:16, at] = f[16:24]
        field_ref[16:24, at] = f[24:32] + 256 * f[32:40]
    for s in range(RUNS):
        fetched[s].wait()
        moved = dot(onehot(SORT, position[s]), payload_ref[SORT * s : SORT * (s + 1), :])
        for j in range(PARTS):
            out_ref[j, part_rows * s : part_rows * (s + 1), :] = moved[
                part_rows * j : part_rows * (j + 1)
            ].astype(BF16)


def sort(core, slot, group, weight, payload):
    return pl.pallas_call(
        sort_kernel,
        out_shape=[
            jax.ShapeDtypeStruct((PARTS, A_DEV // PARTS, D), BF16),
            jax.ShapeDtypeStruct((3 * PARTS, A_DEV // PARTS), I32),
        ],
        in_specs=[SMEM] + [VMEM] * 3 + [HBM],
        out_specs=[VMEM] * 2,
        scratch_shapes=[pltpu.VMEM((A_DEV, D), BF16), pltpu.SemaphoreType.DMA((RUNS,))],
        compiler_params=LIMIT,
        name="sort",
    )(core, *(in_hbm(x.reshape(32, 128)) for x in (slot, group, weight)), in_hbm(payload))


def join_a_kernel(view_ref, *refs):
    db, (sorted_ref, field_ref), (terms_hbm, field_hbm, table_hbm) = refs[:4], refs[4:6], refs[6:9]
    table_ref, rows_ref, sems = refs[9:]
    sent = [pltpu.make_async_copy(field_ref, field_hbm, sems.at[PARTS])]
    for s in range(4):
        at = pl.ds(((view_ref[0] + 4 - s) % 4) * 128, 128)
        sent.append(pltpu.make_async_copy(db[s], table_hbm.at[at], sems.at[PARTS + 1 + s]))
    for copy in sent:
        copy.start()
    fill(table_ref, view_ref[0], lambda s: db[s][...])
    for j in range(PARTS):
        weight = field_ref[PARTS + j : PARTS + j + 1, :].astype(F32)
        rows_ref[j] = terms_of(table_ref, field_ref[j : j + 1, :], weight, sorted_ref[j])
        sent.append(pltpu.make_async_copy(rows_ref.at[j], terms_hbm.at[j], sems.at[j]))
        sent[-1].start()
    for copy in sent:
        copy.wait()


def add_windows(half, total_ref, rows_ref, line_ref, starts, ends):
    base = half * (GROUPS // 2)

    def window(j, at, size):
        chosen = onehot(size, line_ref[j : j + 1, :] - at)
        total_ref[pl.ds(pl.multiple_of(at - base, 64), size), :] += dot(chosen, rows_ref[j])

    near = range(PARTS // 2 * half, PARTS // 2 * (half + 1))
    first = [jnp.clip(start, base, base + GROUPS // 2) for start in starts]
    for j in near:
        window(j, first[j], WINDOW)
    for j in range(PARTS):
        begin = first[j] + (WINDOW if j in near else 0)
        last = jnp.minimum(ends[j], base + GROUPS // 2 - 1)

        def more(i, carry, j=j, begin=begin):
            window(j, begin + i * STEP, STEP)
            return carry

        lax.fori_loop(0, (last - begin + STEP) // STEP, more, 0)


def add_deltas(half, total_ref, place_ref, delta_ref):
    for g in range(2):
        chosen = onehot(1024, place_ref[...] - (half * (GROUPS // 2) + 1024 * g))
        total_ref[1024 * g : 1024 * (g + 1), :] = dot(chosen, delta_ref[...])
    total_ref[GROUPS // 2 :, :] = jnp.zeros((WINDOW, D), F32)


def join_d_kernel(view_ref, core_ref, *refs):
    db_hbm, b, (field_hbm, terms_hbm, in_ref) = refs[0], refs[1:5], refs[5:8]
    peer_ref, delta_ref, place_ref, rows_ref, line_ref, bound_ref = refs[8:14]
    whole_ref, total_ref, db_ref, b_ref, field_ref, sems = refs[14:]
    view, core = view_ref[0], core_ref[0]
    tables = [pltpu.make_async_copy(db_hbm, db_ref, sems.at[0])]
    for s in range(4):
        at = pl.ds(((view + 4 - s) % 4) * 128, 128)
        tables.append(pltpu.make_async_copy(b[s], b_ref.at[at], sems.at[1 + s]))
    fields = pltpu.make_async_copy(field_hbm, field_ref, sems.at[5])
    terms = pltpu.make_async_copy(terms_hbm, rows_ref, sems.at[6])
    for copy in (*tables, fields, terms):
        copy.start()
    slots = []
    for c in range(8):
        slot, group = fields_of(in_ref, c)
        place_ref[:, 256 * c : 256 * (c + 1)] = place_of(group, core)
        slots.append(slot)
    for copy in tables:
        copy.wait()
    whole = b_ref[...] + db_ref[...]
    high = whole.astype(BF16)
    whole_ref[:, :D] = high
    whole_ref[:, D:] = (whole - high.astype(F32)).astype(BF16)
    for c in range(8):
        at = slice(256 * c, 256 * (c + 1))
        delta_ref[at, :] = terms_of(whole_ref, slots[c], None, payload_of(in_ref, c))
    fields.wait()
    starts, ends = [], []
    for j in range(PARTS):
        line = field_ref[2 * PARTS + j : 2 * PARTS + j + 1, :]
        line_ref[j : j + 1, :] = line
        starts.append((jnp.min(line) >> 6) << 6)
        ends.append(jnp.max(line))
        bound_ref[j], bound_ref[PARTS + j] = starts[j], ends[j]
    add_deltas(0, total_ref, place_ref, delta_ref)
    terms.wait()
    add_windows(0, total_ref, rows_ref, line_ref, starts, ends)
    peer_ref[...] = total_ref[: GROUPS // 2, :]


def own_kernel(bound_ref, delta_ref, place_ref, rows_ref, line_ref, out_ref, total_ref):
    add_deltas(1, total_ref, place_ref, delta_ref)
    starts = [bound_ref[j] for j in range(PARTS)]
    ends = [bound_ref[PARTS + j] for j in range(PARTS)]
    add_windows(1, total_ref, rows_ref, line_ref, starts, ends)
    out_ref[...] = total_ref[: GROUPS // 2, :]


def join(view, core, db, b, sorted_rows, received):
    rows = OWNERS * CAP
    table = pltpu.VMEM((KEYS_DEV, 2 * D), BF16)
    total = pltpu.VMEM((GROUPS // 2 + WINDOW, D), F32)
    half = jax.ShapeDtypeStruct((GROUPS // 2, D), F32)
    terms, fields, db_table = pl.pallas_call(
        join_a_kernel,
        out_shape=[
            pltpu.HBM((PARTS, A_DEV // PARTS, D), BF16),
            pltpu.HBM((3 * PARTS, A_DEV // PARTS), I32),
            pltpu.HBM((KEYS_DEV, D), F32),
        ],
        in_specs=[SMEM] + [VMEM] * 6,
        out_specs=[HBM] * 3,
        scratch_shapes=[
            table,
            pltpu.VMEM((PARTS, A_DEV // PARTS, D), BF16),
            pltpu.SemaphoreType.DMA((PARTS + 5,)),
        ],
        compiler_params=LIMIT,
        name="join_a",
    )(view, *db, *sorted_rows)
    peer, delta, place, term_rows, line, bound = pl.pallas_call(
        join_d_kernel,
        out_shape=[
            half,
            jax.ShapeDtypeStruct((rows, D), BF16),
            jax.ShapeDtypeStruct((1, rows), I32),
            jax.ShapeDtypeStruct((PARTS, A_DEV // PARTS, D), BF16),
            jax.ShapeDtypeStruct((PARTS, A_DEV // PARTS), I32),
            jax.ShapeDtypeStruct((2 * PARTS,), I32),
        ],
        in_specs=[SMEM] * 2 + [HBM] * 7 + [VMEM],
        out_specs=[VMEM] * 5 + [SMEM],
        scratch_shapes=[
            table,
            total,
            pltpu.VMEM((KEYS_DEV, D), F32),
            pltpu.VMEM((KEYS_DEV, D), F32),
            pltpu.VMEM((3 * PARTS, A_DEV // PARTS), I32),
            pltpu.SemaphoreType.DMA((7,)),
        ],
        compiler_params=pltpu.CompilerParams(vmem_limit_bytes=28 * 2**20),
        name="join_d",
    )(view, core, *map(in_hbm, (db_table, *b, fields, terms)), received)
    other = lax.ppermute(peer, "keys_2", [(0, 1), (1, 0)])
    own = pl.pallas_call(
        own_kernel,
        out_shape=half,
        in_specs=[SMEM] + [VMEM] * 4,
        out_specs=VMEM,
        scratch_shapes=[total],
        compiler_params=LIMIT,
        name="join_own",
    )(bound, delta, place, term_rows, line)
    return (own + other).astype(BF16)


def exchange(packed):
    blocks = packed.reshape(OWNERS, BLOCK, D)
    return lax.all_to_all(blocks, KEYS, 0, 0, tiled=True).reshape(OWNERS * BLOCK, D)


def shards(
    key_slot,
    a_slot,
    a_group,
    a_weight,
    a_payload,
    b_slot,
    b_weight,
    b_payload,
    da_key,
    da_group,
    da_mult,
    da_payload,
    da_count,
    db_key,
    db_mult,
    db_payload,
    db_count,
):
    me = lax.axis_index(KEYS).astype(I32).reshape(1)
    view = lax.axis_index("view").astype(I32).reshape(1)
    table = key_slot.reshape(128, 128)
    core = lax.axis_index("keys_2").astype(I32).reshape(1)
    db_out = pack(me, db_count, table, db_key, db_mult, None, db_payload)
    da_out = pack(me, da_count, table, da_key, da_mult, da_group, da_payload)
    db_in = exchange(db_out)
    da_in = exchange(da_out)
    b_parts = slices(
        sum_b_kernel,
        view,
        jax.ShapeDtypeStruct,
        b_slot.reshape(32, 128),
        b_weight.reshape(32, 128),
        b_payload,
    )
    b = everyone(own_total(b_parts))
    db = everyone(own_total(slices(sum_db_kernel, view, pltpu.HBM, db_in)))
    sorted_rows = sort(core, a_slot, a_group, a_weight, a_payload)
    partial = join(view, core, db, b, sorted_rows, da_in)
    blocks = partial.reshape(GROUPS // 2 // GROUPS_DEV, GROUPS_DEV, D)
    blocks = lax.all_to_all(blocks, ("keys_0", "keys_1", "view"), 0, 0, tiled=True)
    return jnp.sum(blocks.astype(F32), axis=0)


def solution(mesh):
    split = Mesh(
        mesh.devices.reshape(4, 4, 2, mesh.shape["view"]), ("keys_0", "keys_1", "keys_2", "view")
    )
    one, two = P(KEYS_VIEW), P(KEYS_VIEW, None)
    placed = (
        P(), one, one, one, two, one, one, two, one, one, one, two, one, one, one, two, one,
    )
    return jax.shard_map(shards, mesh=split, in_specs=placed, out_specs=two, check_vma=False)
```

```python
import jax
import jax.numpy as jnp
from jax import lax
from jax.experimental import pallas as pl
from jax.experimental.pallas import tpu as pltpu
from jax.sharding import Mesh
from jax.sharding import PartitionSpec as P


KEYS_DEV = 512
GROUPS_DEV = 32
GROUPS = 4096
DELTA_DEV = 1024
A_DEV = 4096
D = 256
OWNERS = 32
CAP = 64
BLOCK = CAP + 8
SORT, RUNS = 512, 8
PARTS = 8
WINDOW = 1024
STEP = 256
LIMIT = pltpu.CompilerParams(vmem_limit_bytes=16 * 2**20)
KEYS = ("keys_0", "keys_1", "keys_2")
KEYS_VIEW = ("keys_0", "keys_1", "keys_2", "view")
F32, BF16, I32, I16 = jnp.float32, jnp.bfloat16, jnp.int32, jnp.int16
NN = (((1,), (0,)), ((), ()))
NT = (((1,), (1,)), ((), ()))
TN = (((0,), (0,)), ((), ()))
VMEM = pl.BlockSpec(memory_space=pltpu.VMEM)
SMEM = pl.BlockSpec(memory_space=pltpu.SMEM)
HBM = pl.BlockSpec(memory_space=pltpu.HBM)


def in_hbm(x):
    return pltpu.with_memory_space_constraint(x, pltpu.HBM)


def dot(x, y, dims=NN):
    return lax.dot_general(x, y, dims, preferred_element_type=F32)


def rows_of(shape):
    return lax.broadcasted_iota(I32, shape, 0)


def lanes_of(shape):
    return lax.broadcasted_iota(I32, shape, 1)


def flat(x):
    return jnp.concatenate([x[j : j + 1, :] for j in range(x.shape[0])], axis=1)


def pick(condition, value):
    return jnp.where(condition, value, 0.0).astype(BF16)


def onehot(rows, index, value=None):
    hit = lax.broadcasted_iota(I16, (rows, index.shape[1]), 0) == index.astype(I16)
    one = jnp.ones((), BF16) if value is None else value.astype(BF16)
    return jnp.where(hit, one, jnp.zeros((), BF16))


def counted_before(marks):
    step = jnp.where(
        (rows_of((128, 256)) < lanes_of((128, 256))) | (lanes_of((128, 256)) >= 128), 1.0, 0.0
    ).astype(BF16)
    before, carry = [], jnp.zeros((marks.shape[0], 128), F32)
    for j in range(marks.shape[1] // 128):
        counted = dot(marks[:, 128 * j : 128 * (j + 1)].astype(BF16), step)
        before.append(counted[:, :128] + carry)
        carry = carry + counted[:, 128:]
    return jnp.concatenate(before, axis=1)


def pack_kernel(with_group, me_ref, count_ref, table_ref, key_ref, mult_ref, *rest):
    group_ref = rest[0] if with_group else None
    payload_hbm, out_hbm, payload_ref, out_ref, in_sem, out_sems = rest[-6:]
    rows = DELTA_DEV
    fetch = pltpu.make_async_copy(payload_hbm, payload_ref, in_sem)
    fetch.start()
    key = flat(key_ref[...])
    key_hi, key_lo = key >> 7, key & 127
    low = onehot(128, key_lo)
    table = table_ref[...]
    found = dot((table >> 7).astype(F32).astype(BF16), low) * 128.0 + dot(
        (table & 127).astype(F32).astype(BF16), low
    )
    slot = jnp.sum(jnp.where(rows_of((128, rows)) == key_hi, found, 0.0), axis=0, keepdims=True)
    slot = slot.astype(I32)
    owner, local = slot >> 9, slot & 511
    live = lanes_of((1, rows)) < count_ref[0]
    owner = jnp.where(live, owner, -1)
    marks = jnp.where(rows_of((OWNERS, rows)) == owner, 1.0, 0.0)
    rank = jnp.sum(marks * counted_before(marks), axis=0, keepdims=True).astype(I32)
    position = jnp.where(live, owner * CAP + rank, -1)
    sign = flat(mult_ref[...]).astype(F32)
    field = rows_of((8, rows))
    value = jnp.where(field == 0, local & 255, jnp.where(field == 1, local >> 8, 0))
    if with_group:
        group = flat(group_ref[...])
        value = jnp.where(field == 2, group & 255, jnp.where(field == 3, group >> 8, value))
    value = jnp.broadcast_to(value.astype(F32)[None], (OWNERS, 8, rows)).reshape(8 * OWNERS, rows)
    held = pick((rows_of((8 * OWNERS, rows)) >> 3) == owner, value)
    place = onehot(4 * CAP, rank + CAP * (me_ref[0] % 4))
    fields = dot(held, place, NT).astype(BF16)
    for k in range(OWNERS):
        out_ref[pl.ds(k * BLOCK + CAP, 8), :] = fields[8 * k : 8 * k + 8]
    fetch.wait()
    payload, sent = payload_ref[...], []
    for c in range(OWNERS // 4):
        chosen = onehot(4 * CAP, position - 4 * CAP * c, sign)
        packed = dot(chosen, payload).astype(BF16)
        for j in range(4):
            out_ref[pl.ds((4 * c + j) * BLOCK, CAP), :] = packed[CAP * j : CAP * (j + 1)]
        part = pl.ds(4 * c * BLOCK, 4 * BLOCK)
        sent.append(pltpu.make_async_copy(out_ref.at[part], out_hbm.at[part], out_sems.at[c]))
        sent[-1].start()
    for copy in sent:
        copy.wait()


def pack(me, count, table, key, mult, group, payload):
    extra = [] if group is None else [group.reshape(8, 128)]
    return pl.pallas_call(
        lambda *refs: pack_kernel(group is not None, *refs),
        out_shape=pltpu.HBM((OWNERS * BLOCK, D), BF16),
        in_specs=[SMEM, SMEM] + [VMEM] * (3 + len(extra)) + [HBM],
        out_specs=HBM,
        scratch_shapes=[
            pltpu.VMEM((DELTA_DEV, D), BF16),
            pltpu.VMEM((OWNERS * BLOCK, D), BF16),
            pltpu.SemaphoreType.DMA,
            pltpu.SemaphoreType.DMA((OWNERS // 4,)),
        ],
        compiler_params=LIMIT,
        name="pack_a" if extra else "pack_b",
    )(me, count, *map(in_hbm, (table, key.reshape(8, 128), mult.reshape(8, 128), *extra, payload)))


def fields_of(ref, c):
    total = ref[pl.ds(4 * c * BLOCK + CAP, 8), :].astype(F32)
    for j in range(1, 4):
        total = total + ref[pl.ds((4 * c + j) * BLOCK + CAP, 8), :].astype(F32)
    total = total.astype(I32)
    return total[0:1] + 256 * total[1:2], total[2:3] + 256 * total[3:4]


def payload_of(ref, c):
    return jnp.concatenate(
        [ref[pl.ds((4 * c + j) * BLOCK, CAP), :] for j in range(4)], axis=0
    )


def spread(total_ref, view, outs):
    for s in range(4):
        outs[s][...] = total_ref[pl.ds(((view + s) % 4) * 128, 128), :]


def sum_b_kernel(view_ref, slot_ref, weight_ref, payload_ref, *rest):
    outs, total_ref = rest[:4], rest[4]
    total_ref[...] = jnp.zeros_like(total_ref)
    for c in range(4):
        slot = flat(slot_ref[8 * c : 8 * c + 8, :])
        weight = flat(weight_ref[8 * c : 8 * c + 8, :]).astype(F32)
        chosen = onehot(KEYS_DEV, slot, weight)
        total_ref[...] += dot(chosen, payload_ref[1024 * c : 1024 * (c + 1), :])
    spread(total_ref, view_ref[0], outs)


def sum_db_kernel(view_ref, in_ref, *rest):
    outs, total_ref = rest[:4], rest[4]
    total_ref[...] = jnp.zeros_like(total_ref)
    for c in range(8):
        slot, _ = fields_of(in_ref, c)
        total_ref[...] += dot(onehot(KEYS_DEV, slot), payload_of(in_ref, c))
    spread(total_ref, view_ref[0], outs)


def slices(kernel, view, own, *args):
    return pl.pallas_call(
        kernel,
        out_shape=[own((128, D), F32)] + [jax.ShapeDtypeStruct((128, D), F32)] * 3,
        in_specs=[SMEM] + [VMEM] * len(args),
        out_specs=[VMEM] * 4,
        scratch_shapes=[pltpu.VMEM((KEYS_DEV, D), F32)],
        compiler_params=LIMIT,
    )(view, *args)


def shift(x, s):
    return lax.ppermute(x, "view", [(j, (j + s) % 4) for j in range(4)])


def own_total(parts):
    got = [parts[0]] + [shift(parts[s], s) for s in (1, 2, 3)]
    return (got[0] + got[1]) + (got[2] + got[3])


def everyone(x):
    return [x] + [shift(x, s) for s in (1, 2, 3)]


def fill(ref, view, pieces):
    for s in range(4):
        at = pl.ds(((view + 4 - s) % 4) * 128, 128)
        value = pieces(s)
        high = value.astype(BF16)
        ref[at, :D] = high
        ref[at, D:] = (value - high.astype(F32)).astype(BF16)


def terms_of(ref, slot, weight, payload):
    got = dot(onehot(KEYS_DEV, slot, weight), ref[...], TN)
    return (payload.astype(F32) * (got[:, :D] + got[:, D:])).astype(BF16)


def place_of(group, core):
    own = jnp.where(((group >> 7) & 1) == core, GROUPS // 2, 0)
    return own + ((group >> 8) << 7) + (group & 127)


def sort_kernel(
    core_ref, slot_ref, group_ref, weight_ref, payload_hbm, out_ref, field_ref, payload_ref, sems
):
    fetched = []
    for s in range(RUNS):
        part = pl.ds(SORT * s, SORT)
        fetched.append(
            pltpu.make_async_copy(payload_hbm.at[part], payload_ref.at[part], sems.at[s])
        )
        fetched[-1].start()
    buckets, part_rows = GROUPS // 64, SORT // PARTS
    places = place_of(group_ref[...], core_ref[0])

    def run_of(x, s):
        return flat(x[SORT // 128 * s : SORT // 128 * (s + 1), :])

    bucket = [run_of(places, s) >> 6 for s in range(RUNS)]
    number = rows_of((buckets, SORT))
    marks = [jnp.where(number == k, 1.0, 0.0) for k in bucket]
    first = [jnp.sum(jnp.where(k < number, 1.0, 0.0), axis=1, keepdims=True) for k in bucket]
    before = counted_before(jnp.concatenate(marks, axis=0)) + jnp.concatenate(first, axis=0)
    position = [
        jnp.sum(marks[s] * before[buckets * s : buckets * (s + 1)], axis=0, keepdims=True)
        for s in range(RUNS)
    ]
    position = [p.astype(I32) for p in position]
    row, found = rows_of((5 * PARTS, SORT)), []
    for s in range(RUNS):
        slot, weight, place = (run_of(x, s) for x in (slot_ref[...], weight_ref[...], places))
        value = jnp.zeros((5 * PARTS, SORT), I32)
        for q, part in enumerate((slot & 255, slot >> 8, weight, place & 255, place >> 8)):
            value = jnp.where((row >> 3) == q, part, value)
        held = pick((row & 7) == position[s] >> 6, value.astype(F32))
        lane = (position[s] & 63) + part_rows * (s % 2)
        found.append(dot(held, onehot(2 * part_rows, lane), NT))
    for s in range(0, RUNS, 2):
        at = slice(part_rows * s, part_rows * (s + 2))
        f = (found[s] + found[s + 1]).astype(I32)
        field_ref[0:8, at] = f[0:8] + 256 * f[8:16]
        field_ref[8:16, at] = f[16:24]
        field_ref[16:24, at] = f[24:32] + 256 * f[32:40]
    for s in range(RUNS):
        fetched[s].wait()
        moved = dot(onehot(SORT, position[s]), payload_ref[SORT * s : SORT * (s + 1), :])
        for j in range(PARTS):
            out_ref[j, part_rows * s : part_rows * (s + 1), :] = moved[
                part_rows * j : part_rows * (j + 1)
            ].astype(BF16)


def sort(core, slot, group, weight, payload):
    return pl.pallas_call(
        sort_kernel,
        out_shape=[
            jax.ShapeDtypeStruct((PARTS, A_DEV // PARTS, D), BF16),
            jax.ShapeDtypeStruct((3 * PARTS, A_DEV // PARTS), I32),
        ],
        in_specs=[SMEM] + [VMEM] * 3 + [HBM],
        out_specs=[VMEM] * 2,
        scratch_shapes=[pltpu.VMEM((A_DEV, D), BF16), pltpu.SemaphoreType.DMA((RUNS,))],
        compiler_params=LIMIT,
        name="sort",
    )(core, *(in_hbm(x.reshape(32, 128)) for x in (slot, group, weight)), in_hbm(payload))


def join_a_kernel(view_ref, *refs):
    db, b, (sorted_ref, field_ref) = refs[:4], refs[4:8], refs[8:10]
    terms_hbm, field_hbm, whole_hbm, bound_ref = refs[10:14]
    table_ref, whole_ref, rows_ref, sems = refs[14:]
    sent = [pltpu.make_async_copy(field_ref, field_hbm, sems.at[PARTS])]
    sent[0].start()
    fill(table_ref, view_ref[0], lambda s: db[s][...])
    fill(whole_ref, view_ref[0], lambda s: b[s][...] + db[s][...])
    sent.append(pltpu.make_async_copy(whole_ref, whole_hbm, sems.at[PARTS + 1]))
    sent[1].start()
    for j in range(PARTS):
        weight = field_ref[PARTS + j : PARTS + j + 1, :].astype(F32)
        rows_ref[j] = terms_of(table_ref, field_ref[j : j + 1, :], weight, sorted_ref[j])
        sent.append(pltpu.make_async_copy(rows_ref.at[j], terms_hbm.at[j], sems.at[j]))
        sent[-1].start()
    for j in range(PARTS):
        line = field_ref[2 * PARTS + j : 2 * PARTS + j + 1, :]
        bound_ref[j] = (jnp.min(line) >> 6) << 6
        bound_ref[PARTS + j] = jnp.max(line)
    for copy in sent:
        copy.wait()


def add_windows(half, total_ref, rows_ref, line_ref, starts, ends):
    base = half * (GROUPS // 2)

    def window(j, at, size):
        chosen = onehot(size, line_ref[j : j + 1, :] - at)
        total_ref[pl.ds(pl.multiple_of(at - base, 64), size), :] += dot(chosen, rows_ref[j])

    near = range(PARTS // 2 * half, PARTS // 2 * (half + 1))
    first = [jnp.clip(start, base, base + GROUPS // 2) for start in starts]
    for j in near:
        window(j, first[j], WINDOW)
    for j in range(PARTS):
        begin = first[j] + (WINDOW if j in near else 0)
        last = jnp.minimum(ends[j], base + GROUPS // 2 - 1)

        def more(i, carry, j=j, begin=begin):
            window(j, begin + i * STEP, STEP)
            return carry

        lax.fori_loop(0, (last - begin + STEP) // STEP, more, 0)


def add_deltas(half, total_ref, place_ref, delta_ref):
    for g in range(2):
        chosen = onehot(1024, place_ref[...] - (half * (GROUPS // 2) + 1024 * g))
        total_ref[1024 * g : 1024 * (g + 1), :] = dot(chosen, delta_ref[...])
    total_ref[GROUPS // 2 :, :] = jnp.zeros((WINDOW, D), F32)


def bounds(bound_ref):
    return [[bound_ref[h * PARTS + j] for j in range(PARTS)] for h in (0, 1)]


def join_d_kernel(core_ref, *refs):
    bound_hbm, whole_hbm, field_hbm, terms_hbm, in_ref = refs[:5]
    peer_ref, delta_ref, place_ref, rows_ref, line_ref, bound_ref = refs[5:11]
    whole_ref, total_ref, sems = refs[11:]
    lines = field_hbm.at[pl.ds(2 * PARTS, PARTS)]
    copies = [
        pltpu.make_async_copy(source, target, sems.at[n])
        for n, (source, target) in enumerate(
            (
                (whole_hbm, whole_ref),
                (lines, line_ref),
                (bound_hbm, bound_ref),
                (terms_hbm, rows_ref),
            )
        )
    ]
    for copy in copies:
        copy.start()
    slots = []
    for c in range(8):
        slot, group = fields_of(in_ref, c)
        place_ref[:, 256 * c : 256 * (c + 1)] = place_of(group, core_ref[0])
        slots.append(slot)
    copies[0].wait()
    for c in range(8):
        at = slice(256 * c, 256 * (c + 1))
        delta_ref[at, :] = terms_of(whole_ref, slots[c], None, payload_of(in_ref, c))
    add_deltas(0, total_ref, place_ref, delta_ref)
    for copy in copies[1:]:
        copy.wait()
    add_windows(0, total_ref, rows_ref, line_ref, *bounds(bound_ref))
    peer_ref[...] = total_ref[: GROUPS // 2, :]


def own_kernel(bound_ref, delta_ref, place_ref, rows_ref, line_ref, out_ref, total_ref):
    add_deltas(1, total_ref, place_ref, delta_ref)
    add_windows(1, total_ref, rows_ref, line_ref, *bounds(bound_ref))
    out_ref[...] = total_ref[: GROUPS // 2, :]


def join(view, core, db, b, sorted_rows, received):
    rows = OWNERS * CAP
    table = pltpu.VMEM((KEYS_DEV, 2 * D), BF16)
    total = pltpu.VMEM((GROUPS // 2 + WINDOW, D), F32)
    half = jax.ShapeDtypeStruct((GROUPS // 2, D), F32)
    terms, fields, whole, bound = pl.pallas_call(
        join_a_kernel,
        out_shape=[
            pltpu.HBM((PARTS, A_DEV // PARTS, D), BF16),
            pltpu.HBM((3 * PARTS, A_DEV // PARTS), I32),
            pltpu.HBM((KEYS_DEV, 2 * D), BF16),
            pltpu.HBM((2 * PARTS,), I32),
        ],
        in_specs=[SMEM] + [VMEM] * 10,
        out_specs=[HBM] * 3 + [SMEM],
        scratch_shapes=[
            table,
            table,
            pltpu.VMEM((PARTS, A_DEV // PARTS, D), BF16),
            pltpu.SemaphoreType.DMA((PARTS + 2,)),
        ],
        compiler_params=LIMIT,
        name="join_a",
    )(view, *db, *b, *sorted_rows)
    peer, delta, place, term_rows, line, bound = pl.pallas_call(
        join_d_kernel,
        out_shape=[
            half,
            jax.ShapeDtypeStruct((rows, D), BF16),
            jax.ShapeDtypeStruct((1, rows), I32),
            jax.ShapeDtypeStruct((PARTS, A_DEV // PARTS, D), BF16),
            jax.ShapeDtypeStruct((PARTS, A_DEV // PARTS), I32),
            jax.ShapeDtypeStruct((2 * PARTS,), I32),
        ],
        in_specs=[SMEM] + [HBM] * 4 + [VMEM],
        out_specs=[VMEM] * 5 + [SMEM],
        scratch_shapes=[table, total, pltpu.SemaphoreType.DMA((4,))],
        compiler_params=pltpu.CompilerParams(vmem_limit_bytes=28 * 2**20),
        name="join_d",
    )(core, *map(in_hbm, (bound, whole, fields, terms)), received)
    other = lax.ppermute(peer, "keys_2", [(0, 1), (1, 0)])
    own = pl.pallas_call(
        own_kernel,
        out_shape=half,
        in_specs=[SMEM] + [VMEM] * 4,
        out_specs=VMEM,
        scratch_shapes=[total],
        compiler_params=LIMIT,
        name="join_own",
    )(bound, delta, place, term_rows, line)
    return (own + other).astype(BF16)


def exchange(packed):
    blocks = packed.reshape(OWNERS, BLOCK, D)
    return lax.all_to_all(blocks, KEYS, 0, 0, tiled=True).reshape(OWNERS * BLOCK, D)


def shards(
    key_slot,
    a_slot,
    a_group,
    a_weight,
    a_payload,
    b_slot,
    b_weight,
    b_payload,
    da_key,
    da_group,
    da_mult,
    da_payload,
    da_count,
    db_key,
    db_mult,
    db_payload,
    db_count,
):
    me = lax.axis_index(KEYS).astype(I32).reshape(1)
    view = lax.axis_index("view").astype(I32).reshape(1)
    table = key_slot.reshape(128, 128)
    core = lax.axis_index("keys_2").astype(I32).reshape(1)
    db_out = pack(me, db_count, table, db_key, db_mult, None, db_payload)
    da_out = pack(me, da_count, table, da_key, da_mult, da_group, da_payload)
    db_in = exchange(db_out)
    da_in = exchange(da_out)
    b_parts = slices(
        sum_b_kernel,
        view,
        jax.ShapeDtypeStruct,
        b_slot.reshape(32, 128),
        b_weight.reshape(32, 128),
        b_payload,
    )
    b = everyone(own_total(b_parts))
    db = everyone(own_total(slices(sum_db_kernel, view, pltpu.HBM, db_in)))
    sorted_rows = sort(core, a_slot, a_group, a_weight, a_payload)
    partial = join(view, core, db, b, sorted_rows, da_in)
    blocks = partial.reshape(GROUPS // 2 // GROUPS_DEV, GROUPS_DEV, D)
    blocks = lax.all_to_all(blocks, ("keys_0", "keys_1", "view"), 0, 0, tiled=True)
    return jnp.sum(blocks.astype(F32), axis=0)


def solution(mesh):
    split = Mesh(
        mesh.devices.reshape(4, 4, 2, mesh.shape["view"]), ("keys_0", "keys_1", "keys_2", "view")
    )
    one, two = P(KEYS_VIEW), P(KEYS_VIEW, None)
    placed = (
        P(), one, one, one, two, one, one, two, one, one, one, two, one, one, one, two, one,
    )
    return jax.shard_map(shards, mesh=split, in_specs=placed, out_specs=two, check_vma=False)
```

```python
import jax
import jax.numpy as jnp
from jax import lax
from jax.experimental import pallas as pl
from jax.experimental.pallas import tpu as pltpu
from jax.sharding import Mesh
from jax.sharding import PartitionSpec as P


KEYS_DEV = 512
GROUPS_DEV = 32
GROUPS = 4096
DELTA_DEV = 1024
A_DEV = 4096
D = 256
OWNERS = 32
CAP = 64
BLOCK = CAP + 8
SORT, RUNS = 512, 8
PARTS = 8
WINDOW = 1024
STEP = 256
LIMIT = pltpu.CompilerParams(vmem_limit_bytes=16 * 2**20)
KEYS = ("keys_0", "keys_1", "keys_2")
KEYS_VIEW = ("keys_0", "keys_1", "keys_2", "view")
F32, BF16, I32, I16 = jnp.float32, jnp.bfloat16, jnp.int32, jnp.int16
NN = (((1,), (0,)), ((), ()))
NT = (((1,), (1,)), ((), ()))
TN = (((0,), (0,)), ((), ()))
VMEM = pl.BlockSpec(memory_space=pltpu.VMEM)
SMEM = pl.BlockSpec(memory_space=pltpu.SMEM)
HBM = pl.BlockSpec(memory_space=pltpu.HBM)


def in_hbm(x):
    return pltpu.with_memory_space_constraint(x, pltpu.HBM)


def dot(x, y, dims=NN):
    return lax.dot_general(x, y, dims, preferred_element_type=F32)


def rows_of(shape):
    return lax.broadcasted_iota(I32, shape, 0)


def lanes_of(shape):
    return lax.broadcasted_iota(I32, shape, 1)


def flat(x):
    return jnp.concatenate([x[j : j + 1, :] for j in range(x.shape[0])], axis=1)


def pick(condition, value):
    return jnp.where(condition, value, 0.0).astype(BF16)


def onehot(rows, index, value=None):
    hit = lax.broadcasted_iota(I16, (rows, index.shape[1]), 0) == index.astype(I16)
    one = jnp.ones((), BF16) if value is None else value.astype(BF16)
    return jnp.where(hit, one, jnp.zeros((), BF16))


def counted_before(marks):
    step = jnp.where(
        (rows_of((128, 256)) < lanes_of((128, 256))) | (lanes_of((128, 256)) >= 128), 1.0, 0.0
    ).astype(BF16)
    before, carry = [], jnp.zeros((marks.shape[0], 128), F32)
    for j in range(marks.shape[1] // 128):
        counted = dot(marks[:, 128 * j : 128 * (j + 1)].astype(BF16), step)
        before.append(counted[:, :128] + carry)
        carry = carry + counted[:, 128:]
    return jnp.concatenate(before, axis=1)


def route(count, table, key):
    rows = DELTA_DEV
    key_hi, key_lo = key >> 7, key & 127
    low = onehot(128, key_lo)
    found = dot((table >> 7).astype(F32).astype(BF16), low) * 128.0 + dot(
        (table & 127).astype(F32).astype(BF16), low
    )
    slot = jnp.sum(jnp.where(rows_of((128, rows)) == key_hi, found, 0.0), axis=0, keepdims=True)
    slot = slot.astype(I32)
    owner = jnp.where(lanes_of((1, rows)) < count, slot >> 9, -1)
    marks = jnp.where(rows_of((OWNERS, rows)) == owner, 1.0, 0.0)
    rank = jnp.sum(marks * counted_before(marks), axis=0, keepdims=True).astype(I32)
    return owner, slot & 511, rank


def move_rows(owner, rank, sign, payload, block, out_ref, out_hbm, sems):
    position = jnp.where(owner >= 0, owner * CAP + rank, -1)
    sent = []
    for c in range(OWNERS // 4):
        chosen = onehot(4 * CAP, position - 4 * CAP * c, sign)
        packed = dot(chosen, payload).astype(BF16)
        for j in range(4):
            out_ref[pl.ds((4 * c + j) * block, CAP), :] = packed[CAP * j : CAP * (j + 1)]
        part = pl.ds(4 * c * block, 4 * block)
        sent.append(pltpu.make_async_copy(out_ref.at[part], out_hbm.at[part], sems.at[c]))
        sent[-1].start()
    for copy in sent:
        copy.wait()


def held_fields(owner, rank, first, parts, sender):
    rows = DELTA_DEV
    value, field = jnp.zeros((8, rows), I32), rows_of((8, rows))
    for q, part in enumerate(parts):
        value = jnp.where(field == first + q, part, value)
    value = jnp.broadcast_to(value.astype(F32)[None], (OWNERS, 8, rows)).reshape(8 * OWNERS, rows)
    held = pick((rows_of((8 * OWNERS, rows)) >> 3) == owner, value)
    return dot(held, onehot(4 * CAP, rank + CAP * (sender % 4)), NT)


def pack_b_kernel(
    me_ref, count_ref, a_count_ref, table_ref, key_ref, mult_ref, a_key_ref, a_group_ref, payload_hbm,
    out_hbm, payload_ref, out_ref, in_sem, out_sems,
):
    fetch = pltpu.make_async_copy(payload_hbm, payload_ref, in_sem)
    fetch.start()
    table, me = table_ref[...], me_ref[0]
    owner, local, rank = route(count_ref[0], table, flat(key_ref[...]))
    a_owner, a_local, a_rank = route(a_count_ref[0], table, flat(a_key_ref[...]))
    group = flat(a_group_ref[...])
    fields = held_fields(owner, rank, 0, (local & 255, local >> 8), me) + held_fields(
        a_owner, a_rank, 2, (a_local & 255, a_local >> 8, group & 255, group >> 8), me
    )
    fields = fields.astype(BF16)
    for k in range(OWNERS):
        out_ref[pl.ds(k * BLOCK + CAP, 8), :] = fields[8 * k : 8 * k + 8]
    fetch.wait()
    sign = flat(mult_ref[...]).astype(F32)
    move_rows(owner, rank, sign, payload_ref[...], BLOCK, out_ref, out_hbm, out_sems)


def pack_a_kernel(
    count_ref, table_ref, key_ref, mult_ref, payload_hbm, out_hbm, payload_ref, out_ref, in_sem, out_sems
):
    fetch = pltpu.make_async_copy(payload_hbm, payload_ref, in_sem)
    fetch.start()
    owner, _, rank = route(count_ref[0], table_ref[...], flat(key_ref[...]))
    fetch.wait()
    sign = flat(mult_ref[...]).astype(F32)
    move_rows(owner, rank, sign, payload_ref[...], CAP, out_ref, out_hbm, out_sems)


def pack(kernel, block, scalars, *args):
    return pl.pallas_call(
        kernel,
        out_shape=pltpu.HBM((OWNERS * block, D), BF16),
        in_specs=[SMEM] * len(scalars) + [VMEM] * (len(args) - 1) + [HBM],
        out_specs=HBM,
        scratch_shapes=[
            pltpu.VMEM((DELTA_DEV, D), BF16),
            pltpu.VMEM((OWNERS * block, D), BF16),
            pltpu.SemaphoreType.DMA,
            pltpu.SemaphoreType.DMA((OWNERS // 4,)),
        ],
        compiler_params=LIMIT,
    )(*scalars, *map(in_hbm, args))


def fields_of(ref, c):
    total = ref[pl.ds(4 * c * BLOCK + CAP, 8), :].astype(F32)
    for j in range(1, 4):
        total = total + ref[pl.ds((4 * c + j) * BLOCK + CAP, 8), :].astype(F32)
    total = total.astype(I32)
    return [total[q : q + 1] + 256 * total[q + 1 : q + 2] for q in (0, 2, 4)]


def payload_of(ref, c):
    return jnp.concatenate(
        [ref[pl.ds((4 * c + j) * BLOCK, CAP), :] for j in range(4)], axis=0
    )


def spread(total_ref, view, outs):
    for s in range(4):
        outs[s][...] = total_ref[pl.ds(((view + s) % 4) * 128, 128), :]


def sum_b_kernel(view_ref, slot_ref, weight_ref, payload_ref, *rest):
    outs, total_ref = rest[:4], rest[4]
    total_ref[...] = jnp.zeros_like(total_ref)
    for c in range(4):
        slot = flat(slot_ref[8 * c : 8 * c + 8, :])
        weight = flat(weight_ref[8 * c : 8 * c + 8, :]).astype(F32)
        chosen = onehot(KEYS_DEV, slot, weight)
        total_ref[...] += dot(chosen, payload_ref[1024 * c : 1024 * (c + 1), :])
    spread(total_ref, view_ref[0], outs)


def sum_db_kernel(view_ref, in_ref, *rest):
    outs, slot_ref, group_ref, total_ref = rest[:4], rest[4], rest[5], rest[6]
    total_ref[...] = jnp.zeros_like(total_ref)
    for c in range(8):
        slot, slot_ref[c : c + 1, :], group_ref[c : c + 1, :] = fields_of(in_ref, c)
        total_ref[...] += dot(onehot(KEYS_DEV, slot), payload_of(in_ref, c))
    spread(total_ref, view_ref[0], outs)


def slices(kernel, view, own, *args, more=()):
    return pl.pallas_call(
        kernel,
        out_shape=[own((128, D), F32)] + [jax.ShapeDtypeStruct((128, D), F32)] * 3 + list(more),
        in_specs=[SMEM] + [VMEM] * len(args),
        out_specs=[VMEM] * (4 + len(more)),
        scratch_shapes=[pltpu.VMEM((KEYS_DEV, D), F32)],
        compiler_params=LIMIT,
    )(view, *args)


def shift(x, s):
    return lax.ppermute(x, "view", [(j, (j + s) % 4) for j in range(4)])


def own_total(parts):
    got = [parts[0]] + [shift(parts[s], s) for s in (1, 2, 3)]
    return (got[0] + got[1]) + (got[2] + got[3])


def everyone(x):
    return [x] + [shift(x, s) for s in (1, 2, 3)]


def fill(ref, view, pieces):
    for s in range(4):
        at = pl.ds(((view + 4 - s) % 4) * 128, 128)
        value = pieces(s)
        high = value.astype(BF16)
        ref[at, :D] = high
        ref[at, D:] = (value - high.astype(F32)).astype(BF16)


def terms_of(ref, slot, weight, payload):
    got = dot(onehot(KEYS_DEV, slot, weight), ref[...], TN)
    return (payload.astype(F32) * (got[:, :D] + got[:, D:])).astype(BF16)


def place_of(group, core):
    own = jnp.where(((group >> 7) & 1) == core, GROUPS // 2, 0)
    return own + ((group >> 8) << 7) + (group & 127)


def sort_kernel(
    core_ref, slot_ref, group_ref, weight_ref, payload_hbm, out_ref, field_ref, payload_ref, sems
):
    fetched = []
    for s in range(RUNS):
        part = pl.ds(SORT * s, SORT)
        fetched.append(
            pltpu.make_async_copy(payload_hbm.at[part], payload_ref.at[part], sems.at[s])
        )
        fetched[-1].start()
    buckets, part_rows = GROUPS // 64, SORT // PARTS
    places = place_of(group_ref[...], core_ref[0])

    def run_of(x, s):
        return flat(x[SORT // 128 * s : SORT // 128 * (s + 1), :])

    bucket = [run_of(places, s) >> 6 for s in range(RUNS)]
    number = rows_of((buckets, SORT))
    marks = [jnp.where(number == k, 1.0, 0.0) for k in bucket]
    first = [jnp.sum(jnp.where(k < number, 1.0, 0.0), axis=1, keepdims=True) for k in bucket]
    before = counted_before(jnp.concatenate(marks, axis=0)) + jnp.concatenate(first, axis=0)
    position = [
        jnp.sum(marks[s] * before[buckets * s : buckets * (s + 1)], axis=0, keepdims=True)
        for s in range(RUNS)
    ]
    position = [p.astype(I32) for p in position]
    row, found = rows_of((5 * PARTS, SORT)), []
    for s in range(RUNS):
        slot, weight, place = (run_of(x, s) for x in (slot_ref[...], weight_ref[...], places))
        value = jnp.zeros((5 * PARTS, SORT), I32)
        for q, part in enumerate((slot & 255, slot >> 8, weight, place & 255, place >> 8)):
            value = jnp.where((row >> 3) == q, part, value)
        held = pick((row & 7) == position[s] >> 6, value.astype(F32))
        lane = (position[s] & 63) + part_rows * (s % 2)
        found.append(dot(held, onehot(2 * part_rows, lane), NT))
    for s in range(0, RUNS, 2):
        at = slice(part_rows * s, part_rows * (s + 2))
        f = (found[s] + found[s + 1]).astype(I32)
        field_ref[0:8, at] = f[0:8] + 256 * f[8:16]
        field_ref[8:16, at] = f[16:24]
        field_ref[16:24, at] = f[24:32] + 256 * f[32:40]
    for s in range(RUNS):
        fetched[s].wait()
        moved = dot(onehot(SORT, position[s]), payload_ref[SORT * s : SORT * (s + 1), :])
        for j in range(PARTS):
            out_ref[j, part_rows * s : part_rows * (s + 1), :] = moved[
                part_rows * j : part_rows * (j + 1)
            ].astype(BF16)


def sort(core, slot, group, weight, payload):
    return pl.pallas_call(
        sort_kernel,
        out_shape=[
            jax.ShapeDtypeStruct((PARTS, A_DEV // PARTS, D), BF16),
            jax.ShapeDtypeStruct((3 * PARTS, A_DEV // PARTS), I32),
        ],
        in_specs=[SMEM] + [VMEM] * 3 + [HBM],
        out_specs=[VMEM] * 2,
        scratch_shapes=[pltpu.VMEM((A_DEV, D), BF16), pltpu.SemaphoreType.DMA((RUNS,))],
        compiler_params=LIMIT,
        name="sort",
    )(core, *(x.reshape(32, 128) for x in (slot, group, weight)), in_hbm(payload))


def join_a_kernel(view_ref, *refs):
    db, b, (sorted_ref, field_ref) = refs[:4], refs[4:8], refs[8:10]
    terms_hbm, field_hbm, whole_hbm, bound_ref = refs[10:14]
    table_ref, whole_ref, rows_ref, sems = refs[14:]
    sent = [pltpu.make_async_copy(field_ref, field_hbm, sems.at[PARTS])]
    sent[0].start()
    fill(table_ref, view_ref[0], lambda s: db[s][...])
    fill(whole_ref, view_ref[0], lambda s: b[s][...] + db[s][...])
    sent.append(pltpu.make_async_copy(whole_ref, whole_hbm, sems.at[PARTS + 1]))
    sent[1].start()
    for j in range(PARTS):
        weight = field_ref[PARTS + j : PARTS + j + 1, :].astype(F32)
        rows_ref[j] = terms_of(table_ref, field_ref[j : j + 1, :], weight, sorted_ref[j])
        sent.append(pltpu.make_async_copy(rows_ref.at[j], terms_hbm.at[j], sems.at[j]))
        sent[-1].start()
    for j in range(PARTS):
        line = field_ref[2 * PARTS + j : 2 * PARTS + j + 1, :]
        bound_ref[j] = (jnp.min(line) >> 6) << 6
        bound_ref[PARTS + j] = jnp.max(line)
    for copy in sent:
        copy.wait()


def add_windows(half, total_ref, rows_ref, line_ref, starts, ends):
    base = half * (GROUPS // 2)

    def window(j, at, size):
        chosen = onehot(size, line_ref[j : j + 1, :] - at)
        total_ref[pl.ds(pl.multiple_of(at - base, 64), size), :] += dot(chosen, rows_ref[j])

    near = range(PARTS // 2 * half, PARTS // 2 * (half + 1))
    first = [jnp.clip(start, base, base + GROUPS // 2) for start in starts]
    for j in near:
        window(j, first[j], WINDOW)
    for j in range(PARTS):
        begin = first[j] + (WINDOW if j in near else 0)
        last = jnp.minimum(ends[j], base + GROUPS // 2 - 1)

        def more(i, carry, j=j, begin=begin):
            window(j, begin + i * STEP, STEP)
            return carry

        lax.fori_loop(0, (last - begin + STEP) // STEP, more, 0)


def add_deltas(half, total_ref, place_ref, delta_ref):
    for g in range(2):
        chosen = onehot(1024, place_ref[...] - (half * (GROUPS // 2) + 1024 * g))
        total_ref[1024 * g : 1024 * (g + 1), :] = dot(chosen, delta_ref[...])
    total_ref[GROUPS // 2 :, :] = jnp.zeros((WINDOW, D), F32)


def bounds(bound_ref):
    return [[bound_ref[h * PARTS + j] for j in range(PARTS)] for h in (0, 1)]


def join_d_kernel(core_ref, *refs):
    slot_hbm, group_hbm, bound_hbm, whole_hbm, field_hbm, terms_hbm, in_ref = refs[:7]
    peer_ref, delta_ref, place_ref, rows_ref, line_ref, bound_ref = refs[7:13]
    whole_ref, total_ref, slot_ref, group_ref, sems = refs[13:]
    lines = field_hbm.at[pl.ds(2 * PARTS, PARTS)]
    copies = [
        pltpu.make_async_copy(source, target, sems.at[n])
        for n, (source, target) in enumerate(
            (
                (slot_hbm, slot_ref),
                (group_hbm, group_ref),
                (whole_hbm, whole_ref),
                (lines, line_ref),
                (bound_hbm, bound_ref),
                (terms_hbm, rows_ref),
            )
        )
    ]
    for copy in copies:
        copy.start()
    for copy in copies[:3]:
        copy.wait()
    place = place_of(group_ref[...], core_ref[0])
    for c in range(8):
        at = slice(256 * c, 256 * (c + 1))
        place_ref[:, at] = place[c : c + 1, :]
        delta_ref[at, :] = terms_of(whole_ref, slot_ref[c : c + 1, :], None, in_ref[at, :])
    add_deltas(0, total_ref, place_ref, delta_ref)
    for copy in copies[3:]:
        copy.wait()
    add_windows(0, total_ref, rows_ref, line_ref, *bounds(bound_ref))
    peer_ref[...] = total_ref[: GROUPS // 2, :]


def own_kernel(bound_ref, delta_ref, place_ref, rows_ref, line_ref, out_ref, total_ref):
    add_deltas(1, total_ref, place_ref, delta_ref)
    add_windows(1, total_ref, rows_ref, line_ref, *bounds(bound_ref))
    out_ref[...] = total_ref[: GROUPS // 2, :]


def join(view, core, db, b, sorted_rows, received):
    rows = OWNERS * CAP
    table = pltpu.VMEM((KEYS_DEV, 2 * D), BF16)
    total = pltpu.VMEM((GROUPS // 2 + WINDOW, D), F32)
    half = jax.ShapeDtypeStruct((GROUPS // 2, D), F32)
    terms, fields, whole, bound = pl.pallas_call(
        join_a_kernel,
        out_shape=[
            pltpu.HBM((PARTS, A_DEV // PARTS, D), BF16),
            pltpu.HBM((3 * PARTS, A_DEV // PARTS), I32),
            pltpu.HBM((KEYS_DEV, 2 * D), BF16),
            pltpu.HBM((2 * PARTS,), I32),
        ],
        in_specs=[SMEM] + [VMEM] * 10,
        out_specs=[HBM] * 3 + [SMEM],
        scratch_shapes=[
            table,
            table,
            pltpu.VMEM((PARTS, A_DEV // PARTS, D), BF16),
            pltpu.SemaphoreType.DMA((PARTS + 2,)),
        ],
        compiler_params=LIMIT,
        name="join_a",
    )(view, *db, *b, *sorted_rows)
    peer, delta, place, term_rows, line, bound = pl.pallas_call(
        join_d_kernel,
        out_shape=[
            half,
            jax.ShapeDtypeStruct((rows, D), BF16),
            jax.ShapeDtypeStruct((1, rows), I32),
            jax.ShapeDtypeStruct((PARTS, A_DEV // PARTS, D), BF16),
            jax.ShapeDtypeStruct((PARTS, A_DEV // PARTS), I32),
            jax.ShapeDtypeStruct((2 * PARTS,), I32),
        ],
        in_specs=[SMEM] + [HBM] * 6 + [VMEM],
        out_specs=[VMEM] * 5 + [SMEM],
        scratch_shapes=[
            table,
            total,
            pltpu.VMEM((8, 4 * CAP), I32),
            pltpu.VMEM((8, 4 * CAP), I32),
            pltpu.SemaphoreType.DMA((6,)),
        ],
        compiler_params=pltpu.CompilerParams(vmem_limit_bytes=28 * 2**20),
        name="join_d",
    )(core, *map(in_hbm, (*received[:2], bound, whole, fields, terms)), received[2])
    other = lax.ppermute(peer, "keys_2", [(0, 1), (1, 0)])
    own = pl.pallas_call(
        own_kernel,
        out_shape=half,
        in_specs=[SMEM] + [VMEM] * 4,
        out_specs=VMEM,
        scratch_shapes=[total],
        compiler_params=LIMIT,
        name="join_own",
    )(bound, delta, place, term_rows, line)
    return (own + other).astype(BF16)


def exchange(packed):
    blocks = packed.reshape(OWNERS, -1, D)
    return lax.all_to_all(blocks, KEYS, 0, 0, tiled=True).reshape(packed.shape)


def shards(
    key_slot,
    a_slot,
    a_group,
    a_weight,
    a_payload,
    b_slot,
    b_weight,
    b_payload,
    da_key,
    da_group,
    da_mult,
    da_payload,
    da_count,
    db_key,
    db_mult,
    db_payload,
    db_count,
):
    me = lax.axis_index(KEYS).astype(I32).reshape(1)
    view = lax.axis_index("view").astype(I32).reshape(1)
    table = key_slot.reshape(128, 128)
    core = lax.axis_index("keys_2").astype(I32).reshape(1)
    keys = [x.reshape(8, 128) for x in (db_key, db_mult, da_key, da_group, da_mult)]
    db_out = pack(pack_b_kernel, BLOCK, (me, db_count, da_count), table, *keys[:4], db_payload)
    da_out = pack(pack_a_kernel, CAP, (da_count,), table, keys[2], keys[4], da_payload)
    db_in = exchange(db_out)
    da_in = exchange(da_out)
    b_parts = slices(
        sum_b_kernel,
        view,
        jax.ShapeDtypeStruct,
        b_slot.reshape(32, 128),
        b_weight.reshape(32, 128),
        b_payload,
    )
    b = everyone(own_total(b_parts))
    line = pltpu.HBM((8, 4 * CAP), I32)
    *db_parts, da_slot, da_place = slices(sum_db_kernel, view, pltpu.HBM, db_in, more=(line, line))
    db = everyone(own_total(db_parts))
    sorted_rows = sort(core, a_slot, a_group, a_weight, a_payload)
    partial = join(view, core, db, b, sorted_rows, (da_slot, da_place, da_in))
    blocks = partial.reshape(GROUPS // 2 // GROUPS_DEV, GROUPS_DEV, D)
    blocks = lax.all_to_all(blocks, ("keys_0", "keys_1", "view"), 0, 0, tiled=True)
    return jnp.sum(blocks.astype(F32), axis=0)


def solution(mesh):
    split = Mesh(
        mesh.devices.reshape(4, 4, 2, mesh.shape["view"]), ("keys_0", "keys_1", "keys_2", "view")
    )
    one, two = P(KEYS_VIEW), P(KEYS_VIEW, None)
    placed = (
        P(), one, one, one, two, one, one, two, one, one, one, two, one, one, one, two, one,
    )
    return jax.shard_map(shards, mesh=split, in_specs=placed, out_specs=two, check_vma=False)
```
